32 devices in a mesh: role: 4 (over z), grp: 2 (over y), rep: 4 (over x, core).
Axes of the slice: x: 2, y: 2, z: 4, core: 2. Of those that a mesh axis runs over, the one named last changes fastest.
Arguments:
- facets: bfloat16 [4, 2, 4096, 4096], P('role', None, ('grp', 'rep')), may hold values from -6 to 6
- taper: float32 [4, 4096], P('role'), may hold values from 0.3 to 1.5
- kernel: float32 [8], replicated, may hold values from 0.1 to 0.5
- observed: float32 [2, 8, 16, 512], P(None, ('role', 'grp'), 'rep'), may hold values from -6 to 6
- patch_pos: int32 [8, 16], P(('role', 'grp'), 'rep'), may hold values from 0 to 23, as said below
- counts: int32 [8, 16], P(('role', 'grp'), 'rep'), may hold values from 1 to 512, 5120 in all within a row
- vis_u: int32 [8, 16, 512], P(('role', 'grp'), 'rep'), may hold values from 0 to 24
- vis_v: int32 [8, 16, 512], P(('role', 'grp'), 'rep'), may hold values from 0 to 24
Outputs:
- residual_vis: float32 [2, 8, 16, 512], P(None, ('role', 'grp'), 'rep')
- returned: bfloat16 [2, 8, 128, 128], P(None, None, ('grp', 'rep'))
The draws below stay inside these ranges and needn't reach their ends.
Inputs may be any that keep to these rules, and one draw needn't show every extreme that they name: Visibility slots v < counts are live, the rest are padding; the counts of one subgrid's patches sum to 5120 and one of them equals 512. `patch_pos`: split the patches of a subgrid into 4 aligned runs of 4; in each run the first patch covers a block in the first column of blocks and the second a block in the last column of blocks, the others any block.
All inputs are finite; a program needn't handle non-finite values. No bound on the sum of `counts` on one device may be relied on, other than what follows from the above.
Results may differ from the reference program's by a relative error of at most 0.014.
Values may be sent and summed in bfloat16 or wider, within the bound.
No kernel may reach another device: no remote copies, remote signals or barrier semaphores. Data moves between devices by JAX's collectives and lax.ppermute only.
A program may use at most 64 MiB of HBM per device.

```python
import math
import jax
import jax.numpy as jnp
import numpy as np
from jax import lax

F = 4096
C = 128
PATCH = 32
EDGE = 32
KW = 8
KMAX = 512
NP = 16
FACETS = 4
NSX = 8
N_REP = 4


def draw_patch_pos(key, part):
    col_blocks = (C + 2 * EDGE) // PATCH
    row_blocks = C // PATCH
    key_rows = jax.random.fold_in(key, 11)
    key_cols = jax.random.fold_in(key, 23)
    row_pick = jax.random.randint(key_rows, (NSX, NP), 0, row_blocks, dtype=jnp.int32)
    col_pick = jax.random.randint(key_cols, (NSX, NP), 0, col_blocks, dtype=jnp.int32)
    local_index = (jnp.arange(NP, dtype=jnp.int32) % (NP // N_REP))[None, :]
    col_final = jnp.where(local_index == 0, 0, jnp.where(local_index == 1, col_blocks - 1, col_pick))
    return (row_pick * col_blocks + col_final).astype(jnp.int32)


def plant(values, key, least, top_value):
    extent = values.shape
    spot = [jax.random.randint(jax.random.fold_in(key, axis), (), 0, extent[axis]) for axis in range(len(extent))]
    values = values.at[tuple(spot)].set(least)
    longest = extent.index(max(extent))
    spot[longest] = (spot[longest] + 1) % extent[longest]
    return values.at[tuple(spot)].set(top_value)


def steps_of(key, extent, cuts, least, top_value):
    def one(dim, blocks):
        steps = jax.random.uniform(jax.random.fold_in(jax.random.fold_in(key, 6), dim), (blocks,), jnp.float32, least / len(cuts), top_value / len(cuts))
        return jnp.repeat(jnp.exp(steps), extent[dim] // blocks).reshape((-1,) + (1,) * (len(extent) - dim - 1))

    gain = one(*cuts[0])
    for cut in cuts[1:]:
        gain = gain * one(*cut)
    return gain


def profile(number_of, total, bound, slope):
    weights = [(1 << 20) // math.isqrt(rank ** slope) + 1 for rank in range(2, number_of + 1)]
    surplus, holding = total - bound - (number_of - 1), [1] * (number_of - 1)
    while surplus > 0:
        candidates = [i for i in range(number_of - 1) if holding[i] < bound]
        pool, left = sum([weights[i] for i in candidates]), surplus
        for i in candidates:
            addition = min(bound - holding[i], max(1, left * weights[i] // pool), surplus)
            holding[i] = holding[i] + addition
            surplus = surplus - addition
    return np.array([bound] + holding)


def uneven_parts(rng, number_of, total, bound, lean):
    if number_of == 2:
        one = jax.random.randint(rng, (), max(1, total - bound), min(bound, total - 1) + 1)
        return jnp.stack([one, total - one])
    sizes = jnp.asarray(profile(number_of, total, bound, lean), jnp.int32)
    twos = (number_of - 1) // 2
    giver, taker = sizes[1:1 + 2 * twos:2], sizes[2:2 + 2 * twos:2]
    margin = jnp.minimum(giver - 1, bound - taker)
    moved = jax.random.randint(jax.random.fold_in(rng, 1), (twos,), 0, 1 << 20) % (margin + 1)
    sizes = sizes.at[1:1 + 2 * twos:2].set(giver - moved).at[2:2 + 2 * twos:2].set(taker + moved)
    return sizes[jax.random.permutation(jax.random.fold_in(rng, 2), number_of)]


def centred(rng, shape, deviation, most, split=(), held_as=jnp.bfloat16):
    entries = jax.random.normal(rng, shape, jnp.float32) * deviation
    if len(split) > 0:
        entries = steps_of(rng, shape, split, -0.22, 0.18) * entries
    return jnp.clip(entries, min=-most, max=most).astype(held_as)


def setup_inputs(seed: int = 0) -> dict:
    seeds = jax.random.split(jax.random.key(seed), 9)
    return {
        "facets": centred(seeds[0], (FACETS, 2, F, F), 1.0, 6.0, ((0, 4), (2, 8))),
        "taper": jnp.clip(0.3 + 1.2 * jax.random.uniform(seeds[1], (FACETS, F), jnp.float32) ** steps_of(seeds[1], (FACETS, F), ((0, 4),), -0.2, 0.2), 0.3, 1.5),
        "kernel": jnp.clip(jax.random.uniform(seeds[2], (KW,), jnp.float32, 0.1, 0.5), 0.1, 0.5),
        "observed": centred(seeds[3], (2, NSX, NP, KMAX), 1.0, 6.0, ((1, 8), (2, 4)), jnp.float32),
        "patch_pos": draw_patch_pos(jax.random.fold_in(seeds[8], 71), 0),
        "counts": jax.vmap(lambda own: uneven_parts(own, NP, NP * KMAX * 5 // 8, KMAX, 2))(jax.random.split(seeds[5], NSX)).reshape((NSX, NP)).astype(jnp.int32),
        "vis_u": plant(jax.random.randint(seeds[6], (NSX, NP, KMAX), 0, PATCH - KW + 1), jax.random.fold_in(seeds[6], 1), 0, PATCH - KW).astype(jnp.int32),
        "vis_v": plant(jax.random.randint(seeds[7], (NSX, NP, KMAX), 0, PATCH - KW + 1), jax.random.fold_in(seeds[7], 1), 0, PATCH - KW).astype(jnp.int32),
    }


def phases(frequency, length):
    columns = jnp.arange(length, dtype=jnp.int32)
    product = frequency[:, None] * columns[None, :] % length
    angles = product.astype(jnp.float32) * (2.0 * math.pi / length)
    return (jnp.cos(angles), jnp.sin(angles))

def windowed(frequency, window):
    length = window.shape[0]
    wave_cos, wave_sin = phases(frequency, length)
    scale_norm = 1.0 / math.sqrt(length)
    table_re = (window[None, :] * wave_cos * scale_norm).astype(jnp.bfloat16)
    table_im = (-(window[None, :] * wave_sin) * scale_norm).astype(jnp.bfloat16)
    return (table_re, table_im)

def contract(left, right):
    return lax.dot_general(left, right, (((1,), (1,)), ((), ())), preferred_element_type=jnp.float32)

def project(table_re, table_im, data_re, data_im):
    part_re = contract(table_re, data_re) - contract(table_im, data_im)
    part_im = contract(table_re, data_im) + contract(table_im, data_re)
    return (part_re, part_im)

def modulate(part_re, part_im, wave_cos, wave_sin):
    mod_re = (part_re * wave_cos + part_im * wave_sin).astype(jnp.bfloat16)
    mod_im = (part_im * wave_cos - part_re * wave_sin).astype(jnp.bfloat16)
    return (mod_re, mod_im)

def kernel_rows(offsets, kernel):
    cell_index = jnp.arange(PATCH, dtype=jnp.int32)
    distance = cell_index[None, :, None] - offsets[:, None, :]
    result = jnp.zeros(distance.shape, jnp.float32)
    for position in range(KW):
        result = result + kernel[position] * (distance == position).astype(jnp.float32)
    return result

def degrid(widened, patch_pos, counts, vis_u, vis_v, observed, kernel):
    high = lax.Precision.HIGHEST
    row_blocks = widened.shape[1] // PATCH
    col_blocks = widened.shape[2] // PATCH
    blocks = widened.reshape(2, row_blocks, PATCH, col_blocks, PATCH).transpose(0, 1, 3, 2, 4)
    blocks = blocks.reshape(2, row_blocks * col_blocks, PATCH, PATCH)
    selected = jnp.take(blocks, patch_pos, axis=1).astype(jnp.float32)
    rows_u = kernel_rows(vis_u, kernel)
    rows_v = kernel_rows(vis_v, kernel)
    partial_value = jnp.einsum('cpab,pav->cpbv', selected, rows_u, precision=high)
    predicted = jnp.einsum('cpbv,pbv->cpv', partial_value, rows_v, precision=high)
    live_mask = (jnp.arange(observed.shape[-1], dtype=jnp.int32)[None, :] < counts[:, None]).astype(jnp.float32)
    residual = (observed - predicted) * live_mask[None]
    weighted = residual[:, :, None, :] * rows_v[None]
    gridded = jnp.einsum('pav,cpbv->cpab', rows_u, weighted, precision=high)
    one_hot = (patch_pos[:, None] == jnp.arange(row_blocks * col_blocks, dtype=jnp.int32)[None, :]).astype(jnp.float32)
    placed = jnp.einsum('pq,cpab->cqab', one_hot, gridded, precision=high)
    regrid = placed.reshape(2, row_blocks, col_blocks, PATCH, PATCH).transpose(0, 1, 3, 2, 4)
    return (residual, regrid.reshape(2, widened.shape[1], widened.shape[2]))

def reference(facets, taper, kernel, observed, patch_pos, counts, vis_u, vis_v):
    row_freq = jnp.arange(C, dtype=jnp.int32)

    def section_one(pair):
        facet, window = pair
        table_re, table_im = windowed(row_freq, window)
        part_re, part_im = project(table_re, table_im, facet[0], facet[1])
        return jnp.stack([part_re, part_im]).astype(jnp.bfloat16)
    parts = lax.map(section_one, (facets, taper))
    base_re, base_im = windowed(jnp.arange(C, dtype=jnp.int32), jnp.ones((F,), jnp.float32))

    def section_two(column):
        shift_freq = (column * (F // NSX)).astype(jnp.int32).reshape(1)
        wave_cos, wave_sin = phases(shift_freq, F)
        total = jnp.zeros((2, C, C), jnp.float32)
        for facet in range(FACETS):
            window = taper[facet][None, :]
            mod_re, mod_im = modulate(parts[facet, 0].astype(jnp.float32), parts[facet, 1].astype(jnp.float32), window * wave_cos, window * wave_sin)
            q_re, q_im = project(mod_re, mod_im, base_re, base_im)
            contrib = jnp.stack([q_re, q_im]).astype(jnp.bfloat16)
            total = total + contrib.astype(jnp.float32)
        return total.astype(jnp.bfloat16)
    subs = lax.map(section_two, jnp.arange(NSX, dtype=jnp.int32))
    zeros_col = jnp.zeros((1, 2, C, C), jnp.bfloat16)
    left_nb = jnp.concatenate([zeros_col, subs[:-1]], axis=0)[..., C - EDGE:]
    right_nb = jnp.concatenate([subs[1:], zeros_col], axis=0)[..., :EDGE]
    widened = jnp.concatenate([left_nb, subs, right_nb], axis=-1)
    flat_obs = observed.transpose(1, 0, 2, 3)

    def one_subgrid(items):
        wide, pos, cnt, uu, vv, obs = items
        return degrid(wide, pos, cnt, uu, vv, obs, kernel)
    residual, regrid = lax.map(one_subgrid, (widened, patch_pos, counts, vis_u, vis_v, flat_obs))
    residual_vis = residual.transpose(1, 0, 2, 3)
    center = regrid[..., EDGE:EDGE + C]
    zeros_edge = jnp.zeros((1, 2, C, EDGE), jnp.float32)
    from_left = jnp.concatenate([zeros_edge, regrid[:-1, :, :, EDGE + C:]], axis=0)
    from_right = jnp.concatenate([regrid[1:, :, :, :EDGE], zeros_edge], axis=0)
    resid = center.at[..., :EDGE].add(from_left).at[..., C - EDGE:].add(from_right)
    resid = resid.astype(jnp.bfloat16)
    returned = resid.transpose(1, 0, 2, 3)
    return (residual_vis, returned)
```

```python
import math

import jax
import numpy as np
import jax.numpy as jnp
from jax import lax
from jax.experimental import pallas as pl
from jax.experimental.pallas import tpu as pltpu
from jax.sharding import PartitionSpec as P

F = 4096
C = 128
PATCH = 32
EDGE = 32
KW = 8


def extended(block, sides, width):
    for axis, dim in sides:
        count = lax.axis_size(axis)
        forward = [(i, i + 1) for i in range(count - 1)]
        backward = [(target, source) for source, target in forward]
        low = lax.ppermute(
            lax.slice_in_dim(block, block.shape[dim] - width, None, axis=dim), axis, forward
        )
        high = lax.ppermute(lax.slice_in_dim(block, 0, width, axis=dim), axis, backward)
        block = jnp.concatenate([low, block, high], axis=dim)
    return block


def shifted(value, axis, by):
    size = lax.axis_size(axis)
    pairs = [(i, i + by) for i in range(size) if 0 <= i + by < size]
    return lax.ppermute(value, axis, pairs)


def phases(frequency, length):
    columns = jnp.arange(length, dtype=jnp.int32)
    product = frequency[:, None] * columns[None, :] % length
    angles = product.astype(jnp.float32) * (2.0 * math.pi / length)
    return (jnp.cos(angles), jnp.sin(angles))


def windowed(frequency, window):
    length = window.shape[0]
    wave_cos, wave_sin = phases(frequency, length)
    scale_norm = 1.0 / math.sqrt(length)
    table_re = (window[None, :] * wave_cos * scale_norm).astype(jnp.bfloat16)
    table_im = (-(window[None, :] * wave_sin) * scale_norm).astype(jnp.bfloat16)
    return (table_re, table_im)


def contract(left, right):
    return lax.dot_general(
        left, right, (((1,), (1,)), ((), ())), preferred_element_type=jnp.float32
    )


def project(table_re, table_im, data_re, data_im):
    part_re = contract(table_re, data_re) - contract(table_im, data_im)
    part_im = contract(table_re, data_im) + contract(table_im, data_re)
    return (part_re, part_im)


def modulate(part_re, part_im, wave_cos, wave_sin):
    mod_re = (part_re * wave_cos + part_im * wave_sin).astype(jnp.bfloat16)
    mod_im = (part_im * wave_cos - part_re * wave_sin).astype(jnp.bfloat16)
    return (mod_re, mod_im)


def kernel_rows(offsets, kernel):
    cell_index = jnp.arange(PATCH, dtype=jnp.int32)
    distance = cell_index[None, :, None] - offsets[:, None, :]
    result = jnp.zeros(distance.shape, jnp.float32)
    for position in range(KW):
        result = result + kernel[position] * (distance == position).astype(jnp.float32)
    return result


def degrid(widened, patch_pos, counts, vis_u, vis_v, observed, kernel):
    high = lax.Precision.HIGHEST
    row_blocks = widened.shape[1] // PATCH
    col_blocks = widened.shape[2] // PATCH
    blocks = widened.reshape(2, row_blocks, PATCH, col_blocks, PATCH).transpose(0, 1, 3, 2, 4)
    blocks = blocks.reshape(2, row_blocks * col_blocks, PATCH, PATCH)
    selected = jnp.take(blocks, patch_pos, axis=1).astype(jnp.float32)
    rows_u = kernel_rows(vis_u, kernel)
    rows_v = kernel_rows(vis_v, kernel)
    partial_value = jnp.einsum("cpab,pav->cpbv", selected, rows_u, precision=high)
    predicted = jnp.einsum("cpbv,pbv->cpv", partial_value, rows_v, precision=high)
    live_mask = (jnp.arange(observed.shape[-1], dtype=jnp.int32)[None, :] < counts[:, None]).astype(
        jnp.float32
    )
    residual = (observed - predicted) * live_mask[None]
    weighted = residual[:, :, None, :] * rows_v[None]
    gridded = jnp.einsum("pav,cpbv->cpab", rows_u, weighted, precision=high)
    one_hot = (
        patch_pos[:, None] == jnp.arange(row_blocks * col_blocks, dtype=jnp.int32)[None, :]
    ).astype(jnp.float32)
    placed = jnp.einsum("pq,cpab->cqab", one_hot, gridded, precision=high)
    regrid = placed.reshape(2, row_blocks, col_blocks, PATCH, PATCH).transpose(0, 1, 3, 2, 4)
    return (residual, regrid.reshape(2, widened.shape[1], widened.shape[2]))


def local(facets, taper, kernel, observed, patch_pos, counts, vis_u, vis_v):
    grp_count = lax.axis_size("grp")
    rep_count = lax.axis_size("rep")
    role_count = lax.axis_size("role")
    sub_cols = role_count * grp_count
    row_share = C // (grp_count * rep_count)
    strip_data = facets[0]
    window = taper[0]
    row_freq = jnp.arange(C, dtype=jnp.int32)
    table_re, table_im = windowed(row_freq, window)
    part_re, part_im = project(table_re, table_im, strip_data[0], strip_data[1])
    partial_value = jnp.stack([part_re, part_im]).astype(jnp.bfloat16)
    row_block = lax.all_to_all(
        partial_value, ("grp", "rep"), split_axis=1, concat_axis=2, tiled=True
    )
    shift_freq = jnp.arange(sub_cols, dtype=jnp.int32) * (F // sub_cols)
    wave_cos, wave_sin = phases(shift_freq, F)
    mod_re, mod_im = modulate(
        row_block[0][None].astype(jnp.float32),
        row_block[1][None].astype(jnp.float32),
        (window[None, :] * wave_cos)[:, None, :],
        (window[None, :] * wave_sin)[:, None, :],
    )
    base_re, base_im = windowed(jnp.arange(C, dtype=jnp.int32), jnp.ones((F,), jnp.float32))
    q_re, q_im = project(
        mod_re.reshape(sub_cols * row_share, F),
        mod_im.reshape(sub_cols * row_share, F),
        base_re,
        base_im,
    )
    contrib = jnp.stack([q_re, q_im]).astype(jnp.bfloat16).reshape(2, sub_cols, row_share, C)
    arrived = lax.all_to_all(contrib, ("role", "grp"), split_axis=1, concat_axis=2, tiled=True)
    arrived = arrived.reshape(2, role_count, grp_count, row_share, C).astype(jnp.float32)
    quarter = jnp.sum(arrived, axis=1).astype(jnp.bfloat16)
    collected_rows = lax.all_gather(quarter[:, :, None], "rep", axis=2, tiled=True)
    subgrid = collected_rows.reshape(2, C, C)
    widened = extended(subgrid, ((("role", "grp"), 2),), EDGE)
    residual, regrid = degrid(
        widened, patch_pos[0], counts[0], vis_u[0], vis_v[0], observed[:, 0], kernel
    )
    left_part = regrid[:, :, :EDGE]
    right_part = regrid[:, :, EDGE + C :]
    center = regrid[:, :, EDGE : EDGE + C]
    from_right = shifted(left_part.astype(jnp.bfloat16), ("role", "grp"), -1).astype(
        left_part.dtype
    )
    from_left = shifted(right_part.astype(jnp.bfloat16), ("role", "grp"), 1).astype(
        right_part.dtype
    )
    resid = center.at[:, :, :EDGE].add(from_left).at[:, :, C - EDGE :].add(from_right)
    pieces = resid.reshape(2, grp_count * rep_count, row_share, C)
    spread = lax.all_to_all(
        pieces.astype(jnp.bfloat16), ("grp", "rep"), split_axis=1, concat_axis=1, tiled=True
    ).astype(pieces.dtype)
    owned = jnp.sum(spread.reshape(2, grp_count, rep_count, row_share, C), axis=2).astype(
        jnp.bfloat16
    )
    returned = lax.all_gather(owned, "role", axis=1, tiled=True)
    return (residual[:, None], returned)


LANES = 128
HALF = PATCH // 2
SLOTS = LANES // (2 * HALF)
EVERYONE = ("role", "grp", "rep")


def lanes_of(shape):
    return lax.broadcasted_iota(jnp.int32, shape, len(shape) - 1)


def sublanes_of(shape):
    return lax.broadcasted_iota(jnp.int32, shape, len(shape) - 2)


def wave_tables():
    k = np.arange(C)[:, None]
    first = (k * np.arange(LANES)[None, :]) % F * (2.0 * np.pi / F)
    step = np.broadcast_to((k * LANES) % F * (2.0 * np.pi / F), (C, LANES))
    scale = 1.0 / math.sqrt(F)
    start = np.stack([np.cos(first) * scale, np.sin(first) * scale]).astype(np.float32)
    turn = np.stack([np.cos(step), np.sin(step)]).astype(np.float32)
    return start, turn


def eighth(index):
    def cosine(turn):
        turn = turn & 7
        size = jnp.where((turn & 1) == 1, math.sqrt(0.5), jnp.where((turn & 3) == 0, 1.0, 0.0))
        return jnp.where((turn > 2) & (turn < 6), -size, size).astype(jnp.float32)

    return cosine(index), cosine(index + 6)


def rotated(cos, sin, turn_cos, turn_sin):
    return cos * turn_cos - sin * turn_sin, sin * turn_cos + cos * turn_sin


def row_kernel(facets, taper, start, turn, keep, send, data, table_a, table_b, wave, total, sems):
    chunks, parts, count, width = data.shape

    def fetch(chunk):
        lanes = pl.ds(pl.multiple_of(chunk * width, width), width)
        return pltpu.make_async_copy(facets.at[0, :, :, lanes], data.at[chunk], sems.at[chunk])

    for chunk in range(chunks):
        fetch(chunk).start()
    wave[...] = start[...]

    def build(chunk, carry):
        for piece in range(width // LANES):
            offset = pl.multiple_of(chunk * width + piece * LANES, LANES)
            window = taper[:, pl.ds(offset, LANES)]
            columns = slice(piece * LANES, (piece + 1) * LANES)
            for block in range(C // HALF):
                rows = slice(block * HALF, (block + 1) * HALF)
                cos, sin = wave[0, rows, :], wave[1, rows, :]
                re = window * cos
                im = window * sin
                base = (block % 2) * C + (block // 2) * HALF
                low = slice(base, base + HALF)
                high = slice(base + C // 2, base + C // 2 + HALF)
                table_a[chunk, low, columns] = re.astype(jnp.bfloat16)
                table_a[chunk, high, columns] = (-im).astype(jnp.bfloat16)
                table_b[chunk, low, columns] = im.astype(jnp.bfloat16)
                table_b[chunk, high, columns] = re.astype(jnp.bfloat16)
                cos, sin = rotated(cos, sin, turn[0, rows, :], turn[1, rows, :])
                wave[0, rows, :] = cos
                wave[1, rows, :] = sin
        return carry

    lax.fori_loop(0, chunks, build, 0)
    total[...] = jnp.zeros_like(total)

    def multiply(chunk, carry):
        fetch(chunk).wait()
        total[...] += contract(data[chunk, 0], table_a[chunk]) + contract(
            data[chunk, 1], table_b[chunk]
        )
        return carry

    lax.fori_loop(0, chunks, multiply, 0)
    even = lax.rem(lax.axis_index("rep"), 2) == 0
    first, second = total[:, :C], total[:, C:]
    keep[...] = jnp.where(even, first, second).astype(jnp.bfloat16)
    send[...] = jnp.where(even, second, first).astype(jnp.bfloat16)


def column_kernel(
    rep_count, pos, keep, other, taper, start, turn, out, base, mod, sub, wave
):
    count = keep.shape[0]
    sub_cols = mod.shape[1] // LANES
    mine = lax.axis_index("grp") * rep_count + lax.axis_index("rep")
    eight = sublanes_of((HALF, LANES)) & 7
    for part in range(2):
        place = mine if part == 0 else mine + 1 - 2 * lax.rem(mine, 2)
        phase_cos, phase_sin = eighth(eight * place)
        for piece in range(count // LANES):
            offset = pl.multiple_of(place * count + piece * LANES, LANES)
            window = taper[:, pl.ds(offset, LANES)]
            columns = slice(part * count + piece * LANES, part * count + (piece + 1) * LANES)
            for block in range(C // HALF):
                rows = slice(block * HALF, (block + 1) * HALF)
                if piece == 0:
                    cos, sin = rotated(start[0, rows, :], start[1, rows, :], phase_cos, phase_sin)
                else:
                    cos, sin = wave[0, rows, :], wave[1, rows, :]
                base[rows, columns] = (window * cos).astype(jnp.bfloat16)
                base[C + block * HALF : C + (block + 1) * HALF, columns] = (
                    -(window * sin)
                ).astype(jnp.bfloat16)
                cos, sin = rotated(cos, sin, turn[0, rows, :], turn[1, rows, :])
                wave[0, rows, :] = cos
                wave[1, rows, :] = sin
    right = lanes_of((1, LANES)) >= LANES // 2
    waves = [eighth(eight * column) for column in range(sub_cols)]
    for part, ref in enumerate((keep, other)):

        def shift(step, carry):
            rows = pl.ds(pl.multiple_of(step * HALF, HALF), HALF)
            value = ref[rows, :].astype(jnp.float32)
            swapped = pltpu.roll(value, LANES // 2, 1)
            swapped = jnp.where(right, -swapped, swapped)
            target = pl.ds(pl.multiple_of(part * count + step * HALF, HALF), HALF)
            for column in range(sub_cols):
                cos, sin = waves[column]
                mod[target, column * LANES : (column + 1) * LANES] = (
                    value * cos + swapped * sin
                ).astype(jnp.bfloat16)
            return carry

        lax.fori_loop(0, count // HALF, shift, 0, unroll=2)
    zero = jnp.zeros((EDGE, LANES), jnp.float32)
    sub[:EDGE, :] = zero
    sub[EDGE + sub_cols * C :, :] = zero
    for pair in range(sub_cols // 2):
        product = jnp.dot(
            base[...],
            mod[:, pair * 2 * LANES : (pair + 1) * 2 * LANES],
            preferred_element_type=jnp.float32,
        )
        for side in range(2):
            top = product[:C, side * LANES : (side + 1) * LANES]
            low = pltpu.roll(product[C:, side * LANES : (side + 1) * LANES], LANES // 2, 1)
            begin = EDGE + (2 * pair + side) * C
            sub[begin : begin + C, :] = top + jnp.where(right, low, -low)
    slot = (lanes_of((EDGE, LANES)) // HALF) % SLOTS

    def pack(device, carry):
        column = device // rep_count
        total = jnp.zeros((EDGE, LANES), jnp.float32)
        for p in range(SLOTS):
            begin, row = block_of(pos[device, p], column)
            block = sub[pl.ds(begin, EDGE), :]
            block = pltpu.roll(block, ((p - row) * HALF) & (LANES - 1), 1)
            total = jnp.where(slot == p, block, total)
        out[device] = total.astype(jnp.bfloat16)
        return carry

    lax.fori_loop(0, out.shape[0], pack, 0, unroll=4)


def block_of(position, column):
    col_blocks = (C + 2 * EDGE) // PATCH
    row = position // col_blocks
    begin = column * C + (position - row * col_blocks) * PATCH
    return pl.multiple_of(begin, PATCH), row


def degrid_kernel(
    pos, counts, taps, arrived, observed, vis_u, vis_v, residual, out, taps_u, taps_v, weighted
):
    length = observed.shape[-1]
    left = lanes_of((PATCH, LANES)) < LANES // 2
    taps_u[...] = jnp.zeros_like(taps_u)

    def taps_of(offsets):
        distance = sublanes_of((PATCH, length)) - offsets
        value = jnp.zeros((PATCH, length), jnp.float32)
        for position in range(KW):
            value = jnp.where(distance == position, taps[position], value)
        return value

    for p in range(SLOTS):
        span = slice(p * length, (p + 1) * length)
        rows_u = taps_of(vis_u[0, p : p + 1, :])
        high = rows_u.astype(jnp.bfloat16)
        low = (rows_u - high.astype(jnp.float32)).astype(jnp.bfloat16)
        for half in range(2):
            begin = half * (LANES // 2) + p * HALF
            taps_u[begin : begin + HALF, span] = high[half * HALF : (half + 1) * HALF]
            taps_u[LANES + begin : LANES + begin + HALF, span] = low[
                half * HALF : (half + 1) * HALF
            ]
        taps_v[:, span] = taps_of(vis_v[0, p : p + 1, :])
    sums = []
    for half in range(2):
        total = arrived[half].astype(jnp.float32)
        for source in range(half + 2, arrived.shape[0], 2):
            total = total + arrived[source].astype(jnp.float32)
        sums.append(total)
    swapped = [pltpu.roll(total, LANES // 2, 1) for total in sums]
    patch = jnp.concatenate(
        [jnp.where(left, sums[0], swapped[1]), jnp.where(left, swapped[0], sums[1])], axis=0
    ).astype(jnp.bfloat16)
    patch = jnp.concatenate([patch, patch], axis=1)
    for p in range(SLOTS):
        span = slice(p * length, (p + 1) * length)
        inner = jnp.dot(patch, taps_u[:, span], preferred_element_type=jnp.float32)
        rows_v = taps_v[:, span]
        live = lanes_of((1, length)) < counts[0, p]
        for c in range(2):
            predicted = jnp.sum(inner[c * PATCH : (c + 1) * PATCH] * rows_v, axis=0, keepdims=True)
            value = jnp.where(live, observed[c, 0, p : p + 1, :] - predicted, 0.0)
            residual[c, 0, p : p + 1, :] = value
            value = value * rows_v
            high = value.astype(jnp.bfloat16)
            weighted[c * PATCH : (c + 1) * PATCH, span] = high
            weighted[2 * PATCH + c * PATCH : 2 * PATCH + (c + 1) * PATCH, span] = (
                value - high.astype(jnp.float32)
            ).astype(jnp.bfloat16)
    product = contract(weighted[...], taps_u[...])
    product = product[: 2 * PATCH] + product[2 * PATCH :]
    gridded = product[:, :LANES] + product[:, LANES:]
    parts = [gridded[:PATCH], gridded[PATCH:]]
    swapped = [pltpu.roll(part, LANES // 2, 1) for part in parts]
    halves = [jnp.where(left, parts[0], swapped[1]), jnp.where(left, swapped[0], parts[1])]
    slot = (lanes_of((PATCH, LANES)) // HALF) % SLOTS
    row_of = jnp.zeros((PATCH, LANES), jnp.int32)
    for p in range(SLOTS):
        row_of = jnp.where(slot == p, block_of(pos[0, p], 0)[1], row_of)
    owners = C // HALF
    for owner in range(owners):
        piece = jnp.where(row_of == owner // 2, halves[owner % 2], 0.0).astype(jnp.bfloat16)
        for first in range(0, out.shape[0], owners):
            out[first + owner] = piece


def return_kernel(rep_count, pos, arrived, returned, *scratch):
    sub_cols = returned.shape[1]
    for ref in scratch:
        ref[...] = jnp.zeros_like(ref)

    def place(device, carry):
        value = arrived[device].astype(jnp.float32)
        for p in range(SLOTS):
            begin, _ = block_of(pos[device, p], device // rep_count)
            scratch[p][pl.ds(begin, EDGE), :] += value
        return carry

    lax.fori_loop(0, arrived.shape[0], place, 0, unroll=4)
    shape = (2 * HALF, LANES)
    row, lane = sublanes_of(shape), lanes_of(shape)
    picked = (row // HALF == lane // (LANES // 2)) & (row % HALF == lane % HALF)
    pick = jnp.where(picked, 1.0, 0.0).astype(jnp.bfloat16)
    slot = (lanes_of((C, LANES)) // HALF) % SLOTS
    for column in range(sub_cols):
        rows = slice(EDGE + column * C, EDGE + (column + 1) * C)
        total = scratch[0][rows, :]
        for p in range(1, SLOTS):
            total = jnp.where(slot == p, scratch[p][rows, :], total)
        high = total.astype(jnp.bfloat16)
        low = (total - high.astype(jnp.float32)).astype(jnp.bfloat16)
        value = (contract(pick, high) + contract(pick, low)).astype(jnp.bfloat16)
        for c in range(2):
            returned[c, column] = value[c * HALF : (c + 1) * HALF]


def vmem():
    return pl.BlockSpec(memory_space=pltpu.VMEM)


def smem():
    return pl.BlockSpec(memory_space=pltpu.SMEM)


def fused(facets, taper, kernel, observed, patch_pos, counts, vis_u, vis_v):
    grp_count = lax.axis_size("grp")
    rep_count = lax.axis_size("rep")
    role_count = lax.axis_size("role")
    sub_cols = role_count * grp_count
    devices = sub_cols * rep_count
    count = facets.shape[2]
    length = observed.shape[-1]
    chunks = 8
    width = F // chunks
    start, turn = wave_tables()
    pos = lax.all_to_all(
        jnp.broadcast_to(patch_pos, (devices, SLOTS)),
        EVERYONE,
        split_axis=0,
        concat_axis=0,
        tiled=True,
    )
    strip = jax.ShapeDtypeStruct((count, LANES), jnp.bfloat16)
    keep, send = pl.pallas_call(
        row_kernel,
        out_shape=(strip, strip),
        in_specs=[pl.BlockSpec(memory_space=pl.ANY), vmem(), vmem(), vmem()],
        out_specs=(vmem(), vmem()),
        scratch_shapes=[
            pltpu.VMEM((chunks, 2, count, width), jnp.bfloat16),
            pltpu.VMEM((chunks, 2 * C, width), jnp.bfloat16),
            pltpu.VMEM((chunks, 2 * C, width), jnp.bfloat16),
            pltpu.VMEM((2, C, LANES), jnp.float32),
            pltpu.VMEM((count, 2 * C), jnp.float32),
            pltpu.SemaphoreType.DMA((chunks,)),
        ],
        cost_estimate=pl.CostEstimate(
            flops=8 * C * F * count, bytes_accessed=4 * F * count, transcendentals=0
        ),
        name="rows",
    )(facets, taper, start, turn)
    pairs = [(i, i + 1 - 2 * (i % 2)) for i in range(rep_count)]
    other = lax.ppermute(send, "rep", pairs)
    chunk = jax.ShapeDtypeStruct((devices, PATCH, LANES), jnp.bfloat16)
    padded = sub_cols * C + 2 * EDGE
    outgoing = pl.pallas_call(
        lambda *refs: column_kernel(rep_count, *refs),
        out_shape=chunk,
        in_specs=[smem()] + [vmem()] * 5,
        out_specs=vmem(),
        scratch_shapes=[
            pltpu.VMEM((2 * C, 2 * count), jnp.bfloat16),
            pltpu.VMEM((2 * count, sub_cols * LANES), jnp.bfloat16),
            pltpu.VMEM((padded, LANES), jnp.float32),
            pltpu.VMEM((2, C, LANES), jnp.float32),
        ],
        cost_estimate=pl.CostEstimate(
            flops=8 * C * C * count * sub_cols, bytes_accessed=1 << 20, transcendentals=0
        ),
        name="columns",
    )(pos, keep, other, taper, start, turn)
    arrived = lax.all_to_all(outgoing, EVERYONE, split_axis=0, concat_axis=0, tiled=True)
    residual, gridded = pl.pallas_call(
        degrid_kernel,
        out_shape=(jax.ShapeDtypeStruct(observed.shape, jnp.float32), chunk),
        in_specs=[smem()] * 3 + [vmem()] * 4,
        out_specs=(vmem(), vmem()),
        scratch_shapes=[
            pltpu.VMEM((2 * LANES, SLOTS * length), jnp.bfloat16),
            pltpu.VMEM((PATCH, SLOTS * length), jnp.float32),
            pltpu.VMEM((4 * PATCH, SLOTS * length), jnp.bfloat16),
        ],
        cost_estimate=pl.CostEstimate(
            flops=1 << 28, bytes_accessed=1 << 20, transcendentals=0
        ),
        name="degrid",
    )(patch_pos, counts, kernel, arrived, observed, vis_u, vis_v)
    spread = lax.all_to_all(gridded, EVERYONE, split_axis=0, concat_axis=0, tiled=True)
    returned = pl.pallas_call(
        lambda *refs: return_kernel(rep_count, *refs),
        out_shape=jax.ShapeDtypeStruct((2, sub_cols, HALF, C), jnp.bfloat16),
        in_specs=[smem(), vmem()],
        out_specs=vmem(),
        scratch_shapes=[pltpu.VMEM((padded, LANES), jnp.float32)] * SLOTS,
        cost_estimate=pl.CostEstimate(
            flops=1 << 26, bytes_accessed=1 << 20, transcendentals=0
        ),
        name="returned",
    )(pos, spread)
    return (residual, returned)


def part(facets, taper, kernel, observed, patch_pos, counts, vis_u, vis_v):
    grp_count = lax.axis_size("grp")
    rep_count = lax.axis_size("rep")
    owners = grp_count * rep_count
    sub_cols = lax.axis_size("role") * grp_count
    whole = (
        owners * HALF == C
        and owners == 8
        and sub_cols == 8
        and rep_count % 2 == 0
        and patch_pos.shape[1] == SLOTS
        and facets.shape[2] % LANES == 0
        and observed.shape[-1] % LANES == 0
    )
    path = fused if whole else local
    return path(facets, taper, kernel, observed, patch_pos, counts, vis_u, vis_v)


def solution(mesh):
    return jax.shard_map(
        part,
        mesh=mesh,
        in_specs=(
            P("role", None, ("grp", "rep"), None),
            P("role", None),
            P(),
            P(None, ("role", "grp"), "rep", None),
            P(("role", "grp"), "rep"),
            P(("role", "grp"), "rep"),
            P(("role", "grp"), "rep", None),
            P(("role", "grp"), "rep", None),
        ),
        out_specs=(P(None, ("role", "grp"), "rep", None), P(None, None, ("grp", "rep"), None)),
        check_vma=False,
    )
```

```python
import math

import jax
import numpy as np
import jax.numpy as jnp
from jax import lax
from jax.experimental import pallas as pl
from jax.experimental.pallas import tpu as pltpu
from jax.sharding import PartitionSpec as P


F = 4096
C = 128
PATCH = 32
EDGE = 32
KW = 8


def extended(block, sides, width):
    for axis, dim in sides:
        count = lax.axis_size(axis)
        forward = [(i, i + 1) for i in range(count - 1)]
        backward = [(target, source) for source, target in forward]
        low = lax.ppermute(
            lax.slice_in_dim(block, block.shape[dim] - width, None, axis=dim), axis, forward
        )
        high = lax.ppermute(lax.slice_in_dim(block, 0, width, axis=dim), axis, backward)
        block = jnp.concatenate([low, block, high], axis=dim)
    return block


def shifted(value, axis, by):
    size = lax.axis_size(axis)
    pairs = [(i, i + by) for i in range(size) if 0 <= i + by < size]
    return lax.ppermute(value, axis, pairs)


def phases(frequency, length):
    columns = jnp.arange(length, dtype=jnp.int32)
    product = frequency[:, None] * columns[None, :] % length
    angles = product.astype(jnp.float32) * (2.0 * math.pi / length)
    return (jnp.cos(angles), jnp.sin(angles))


def windowed(frequency, window):
    length = window.shape[0]
    wave_cos, wave_sin = phases(frequency, length)
    scale_norm = 1.0 / math.sqrt(length)
    table_re = (window[None, :] * wave_cos * scale_norm).astype(jnp.bfloat16)
    table_im = (-(window[None, :] * wave_sin) * scale_norm).astype(jnp.bfloat16)
    return (table_re, table_im)


def contract(left, right):
    return lax.dot_general(
        left, right, (((1,), (1,)), ((), ())), preferred_element_type=jnp.float32
    )


def project(table_re, table_im, data_re, data_im):
    part_re = contract(table_re, data_re) - contract(table_im, data_im)
    part_im = contract(table_re, data_im) + contract(table_im, data_re)
    return (part_re, part_im)


def modulate(part_re, part_im, wave_cos, wave_sin):
    mod_re = (part_re * wave_cos + part_im * wave_sin).astype(jnp.bfloat16)
    mod_im = (part_im * wave_cos - part_re * wave_sin).astype(jnp.bfloat16)
    return (mod_re, mod_im)


def kernel_rows(offsets, kernel):
    cell_index = jnp.arange(PATCH, dtype=jnp.int32)
    distance = cell_index[None, :, None] - offsets[:, None, :]
    result = jnp.zeros(distance.shape, jnp.float32)
    for position in range(KW):
        result = result + kernel[position] * (distance == position).astype(jnp.float32)
    return result


def degrid(widened, patch_pos, counts, vis_u, vis_v, observed, kernel):
    high = lax.Precision.HIGHEST
    row_blocks = widened.shape[1] // PATCH
    col_blocks = widened.shape[2] // PATCH
    blocks = widened.reshape(2, row_blocks, PATCH, col_blocks, PATCH).transpose(0, 1, 3, 2, 4)
    blocks = blocks.reshape(2, row_blocks * col_blocks, PATCH, PATCH)
    selected = jnp.take(blocks, patch_pos, axis=1).astype(jnp.float32)
    rows_u = kernel_rows(vis_u, kernel)
    rows_v = kernel_rows(vis_v, kernel)
    partial_value = jnp.einsum("cpab,pav->cpbv", selected, rows_u, precision=high)
    predicted = jnp.einsum("cpbv,pbv->cpv", partial_value, rows_v, precision=high)
    live_mask = (jnp.arange(observed.shape[-1], dtype=jnp.int32)[None, :] < counts[:, None]).astype(
        jnp.float32
    )
    residual = (observed - predicted) * live_mask[None]
    weighted = residual[:, :, None, :] * rows_v[None]
    gridded = jnp.einsum("pav,cpbv->cpab", rows_u, weighted, precision=high)
    one_hot = (
        patch_pos[:, None] == jnp.arange(row_blocks * col_blocks, dtype=jnp.int32)[None, :]
    ).astype(jnp.float32)
    placed = jnp.einsum("pq,cpab->cqab", one_hot, gridded, precision=high)
    regrid = placed.reshape(2, row_blocks, col_blocks, PATCH, PATCH).transpose(0, 1, 3, 2, 4)
    return (residual, regrid.reshape(2, widened.shape[1], widened.shape[2]))


def local(facets, taper, kernel, observed, patch_pos, counts, vis_u, vis_v):
    grp_count = lax.axis_size("grp")
    rep_count = lax.axis_size("rep")
    role_count = lax.axis_size("role")
    sub_cols = role_count * grp_count
    row_share = C // (grp_count * rep_count)
    strip_data = facets[0]
    window = taper[0]
    row_freq = jnp.arange(C, dtype=jnp.int32)
    table_re, table_im = windowed(row_freq, window)
    part_re, part_im = project(table_re, table_im, strip_data[0], strip_data[1])
    partial_value = jnp.stack([part_re, part_im]).astype(jnp.bfloat16)
    row_block = lax.all_to_all(
        partial_value, ("grp", "rep"), split_axis=1, concat_axis=2, tiled=True
    )
    shift_freq = jnp.arange(sub_cols, dtype=jnp.int32) * (F // sub_cols)
    wave_cos, wave_sin = phases(shift_freq, F)
    mod_re, mod_im = modulate(
        row_block[0][None].astype(jnp.float32),
        row_block[1][None].astype(jnp.float32),
        (window[None, :] * wave_cos)[:, None, :],
        (window[None, :] * wave_sin)[:, None, :],
    )
    base_re, base_im = windowed(jnp.arange(C, dtype=jnp.int32), jnp.ones((F,), jnp.float32))
    q_re, q_im = project(
        mod_re.reshape(sub_cols * row_share, F),
        mod_im.reshape(sub_cols * row_share, F),
        base_re,
        base_im,
    )
    contrib = jnp.stack([q_re, q_im]).astype(jnp.bfloat16).reshape(2, sub_cols, row_share, C)
    arrived = lax.all_to_all(contrib, ("role", "grp"), split_axis=1, concat_axis=2, tiled=True)
    arrived = arrived.reshape(2, role_count, grp_count, row_share, C).astype(jnp.float32)
    quarter = jnp.sum(arrived, axis=1).astype(jnp.bfloat16)
    collected_rows = lax.all_gather(quarter[:, :, None], "rep", axis=2, tiled=True)
    subgrid = collected_rows.reshape(2, C, C)
    widened = extended(subgrid, ((("role", "grp"), 2),), EDGE)
    residual, regrid = degrid(
        widened, patch_pos[0], counts[0], vis_u[0], vis_v[0], observed[:, 0], kernel
    )
    left_part = regrid[:, :, :EDGE]
    right_part = regrid[:, :, EDGE + C :]
    center = regrid[:, :, EDGE : EDGE + C]
    from_right = shifted(left_part.astype(jnp.bfloat16), ("role", "grp"), -1).astype(
        left_part.dtype
    )
    from_left = shifted(right_part.astype(jnp.bfloat16), ("role", "grp"), 1).astype(
        right_part.dtype
    )
    resid = center.at[:, :, :EDGE].add(from_left).at[:, :, C - EDGE :].add(from_right)
    pieces = resid.reshape(2, grp_count * rep_count, row_share, C)
    spread = lax.all_to_all(
        pieces.astype(jnp.bfloat16), ("grp", "rep"), split_axis=1, concat_axis=1, tiled=True
    ).astype(pieces.dtype)
    owned = jnp.sum(spread.reshape(2, grp_count, rep_count, row_share, C), axis=2).astype(
        jnp.bfloat16
    )
    returned = lax.all_gather(owned, "role", axis=1, tiled=True)
    return (residual[:, None], returned)


LANES = 128
HALF = PATCH // 2
SLOTS = LANES // (2 * HALF)
TURN = 8
EVERYONE = ("role", "grp", "rep")


def lanes_of(shape):
    return lax.broadcasted_iota(jnp.int32, shape, len(shape) - 1)


def sublanes_of(shape):
    return lax.broadcasted_iota(jnp.int32, shape, len(shape) - 2)


def near(value):
    return pltpu.with_memory_space_constraint(value, pltpu.VMEM)


def far(value):
    return pltpu.with_memory_space_constraint(value, pltpu.HBM)


def waves(cells, scale):
    angles = np.arange(C)[:, None] * cells[None, :] % F * (2.0 * np.pi / F)
    return np.stack([np.cos(angles) * scale, np.sin(angles) * scale]).astype(np.float32)


def row_tables():
    cells = np.arange(LANES)
    return waves(cells, 1.0 / math.sqrt(F)), waves(np.full(LANES, LANES), 1.0)


def column_tables():
    cells = np.arange(LANES) % (LANES // 2) * TURN
    return waves(cells, 1.0 / math.sqrt(F)), waves(np.ones(LANES, np.int64), 1.0)


def eighth(index):
    def cosine(turn):
        turn = turn & 7
        size = jnp.where((turn & 1) == 1, math.sqrt(0.5), jnp.where((turn & 3) == 0, 1.0, 0.0))
        return jnp.where((turn > 2) & (turn < 6), -size, size).astype(jnp.float32)

    return cosine(index), cosine(index + 6)


def rotated(cos, sin, turn_cos, turn_sin):
    return cos * turn_cos - sin * turn_sin, sin * turn_cos + cos * turn_sin


def place_kernel(positions, place, copies):
    col_blocks = (C + 2 * EDGE) // PATCH
    slot = (lanes_of((1, LANES)) // HALF) % SLOTS
    value = jnp.zeros((1, LANES), jnp.int32)
    for p in range(SLOTS):
        value = jnp.where(slot == p, positions[0:1, p : p + 1], value)
    row = sum(jnp.where(value >= block * col_blocks, 1, 0) for block in range(1, C // PATCH))
    value = row * (8 - col_blocks) + value
    place[...] = value
    copies[...] = jnp.broadcast_to(value[None], copies.shape)


def row_kernel(
    rep_count, facets, taper_far, start_far, turn_far, keep, send, data, table_a, table_b,
    wave, turn, taper, total, strip, first_rows, second_rows, sems, small_sems,
):
    chunks, _, width = table_a.shape
    count = keep.shape[0]

    def fetch(chunk):
        columns = pl.ds(pl.multiple_of(chunk * width, width), width)
        return pltpu.make_async_copy(
            facets.at[0, :, :, columns], data.at[chunk], sems.at[chunk]
        )

    small = [
        pltpu.make_async_copy(source, target, small_sems.at[index])
        for index, (source, target) in enumerate(
            ((start_far, wave), (turn_far, turn), (taper_far, taper))
        )
    ]
    for copy in small:
        copy.start()
    fetch(0).start()
    total[...] = jnp.zeros_like(total)
    for copy in small:
        copy.wait()
    fetch(1).start()

    def build(step, carry):
        chunk, piece = step // (width // LANES), step % (width // LANES)
        window = taper[:, pl.ds(pl.multiple_of(step * LANES, LANES), LANES)]
        columns = pl.ds(pl.multiple_of(piece * LANES, LANES), LANES)
        for block in range(C // HALF):
            rows = slice(block * HALF, (block + 1) * HALF)
            cos, sin = wave[0, rows, :], wave[1, rows, :]
            re = window * cos
            im = window * sin
            base = (block % 2) * C + (block // 2) * HALF
            low = slice(base, base + HALF)
            high = slice(base + C // 2, base + C // 2 + HALF)
            table_a[chunk, low, columns] = re.astype(jnp.bfloat16)
            table_a[chunk, high, columns] = (-im).astype(jnp.bfloat16)
            table_b[chunk, low, columns] = im.astype(jnp.bfloat16)
            table_b[chunk, high, columns] = re.astype(jnp.bfloat16)
            cos, sin = rotated(cos, sin, turn[0, rows, :], turn[1, rows, :])
            wave[0, rows, :] = cos
            wave[1, rows, :] = sin
        return carry

    lax.fori_loop(0, chunks * (width // LANES), build, 0)

    def multiply(chunk, carry):
        fetch(chunk).wait()

        @pl.when(chunk + 2 < chunks)
        def _():
            fetch(chunk + 2).start()

        total[...] += contract(data[chunk, 0], table_a[chunk]) + contract(
            data[chunk, 1], table_b[chunk]
        )
        return carry

    lax.fori_loop(0, chunks, multiply, 0)
    place = lax.axis_index("grp") * rep_count + lax.axis_index("rep")
    for piece in range(count // LANES):
        offset = pl.multiple_of(place * count + piece * LANES, LANES)
        strip[piece : piece + 1, :] = taper[:, pl.ds(offset, LANES)]
    window = jnp.transpose(strip[...])
    for piece in range(count // LANES):
        rows = slice(piece * LANES, (piece + 1) * LANES)
        scaled = total[rows, :] * window[:, piece : piece + 1]
        first_rows[rows, :] = scaled[:, :C]
        second_rows[rows, :] = scaled[:, C:]
    even = lax.rem(lax.axis_index("rep"), 2) == 0
    part = count // TURN
    for turned in range(TURN):
        rows = pl.ds(turned, part, stride=TURN)
        first, second = first_rows[rows, :], second_rows[rows, :]
        target = slice(turned * part, (turned + 1) * part)
        keep[target, :] = jnp.where(even, first, second).astype(jnp.bfloat16)
        send[target, :] = jnp.where(even, second, first).astype(jnp.bfloat16)


def column_kernel(rep_count, keep, other, start, turn, sub, base, data, groups):
    part = keep.shape[0] // TURN
    mine = lax.axis_index("grp") * rep_count + lax.axis_index("rep")
    near_by = mine + 1 - 2 * lax.rem(mine, 2)
    shape = (HALF, LANES)
    right = lanes_of((1, LANES)) >= LANES // 2
    place = jnp.where(lanes_of(shape) < LANES // 2, mine, near_by)
    phase_cos, phase_sin = eighth((sublanes_of(shape) & 7) * place)
    for block in range(C // HALF):
        rows = slice(block * HALF, (block + 1) * HALF)
        cos, sin = rotated(start[0, rows, :], start[1, rows, :], phase_cos, phase_sin)
        for turned in range(TURN):
            base[turned, rows, :LANES] = cos.astype(jnp.bfloat16)
            base[turned, rows, LANES:] = sin.astype(jnp.bfloat16)
            if turned < TURN - 1:
                cos, sin = rotated(cos, sin, turn[0, rows, :], turn[1, rows, :])
    for turned in range(TURN):
        source = slice(turned * part, (turned + 1) * part)
        for side, ref in enumerate((keep, other)):
            value = ref[source, :]
            swapped = pltpu.roll(value.astype(jnp.float32), LANES // 2, 1)
            data[turned, side * part : (side + 1) * part, :] = value
            data[turned, (2 + side) * part : (3 + side) * part, :] = jnp.where(
                right, -swapped, swapped
            ).astype(jnp.bfloat16)
    for turned in range(TURN):
        groups[turned] = jnp.dot(base[turned], data[turned], preferred_element_type=jnp.float32)

    def quarter(value):
        swapped = pltpu.roll(value, LANES // 2, 1)
        return jnp.where(right, -swapped, swapped)

    def fourths(values):
        low, high = values[0] + values[2], values[0] - values[2]
        odd, turned = values[1] + values[3], quarter(values[1] - values[3])
        return low + odd, high + turned, low - odd, high - turned

    zero = jnp.zeros((EDGE, LANES), jnp.float32)
    sub[:EDGE, :] = zero
    sub[EDGE + TURN * C :, :] = zero
    size = math.sqrt(0.5)
    for block in range(C // HALF):
        rows = slice(block * HALF, (block + 1) * HALF)
        evens = fourths([groups[turned, rows, :] for turned in range(0, TURN, 2)])
        odds = fourths([groups[turned, rows, :] for turned in range(1, TURN, 2)])
        second, fourth = quarter(odds[1]), quarter(odds[3])
        twisted = (
            odds[0],
            (odds[1] + second) * size,
            quarter(odds[2]),
            (fourth - odds[3]) * size,
        )
        for column in range(TURN // 2):
            for sign in range(2):
                value = evens[column] - twisted[column] if sign else evens[column] + twisted[column]
                begin = EDGE + (column + sign * TURN // 2) * C + block * HALF
                sub[begin : begin + HALF, :] = value


def pack_kernel(rep_count, places, sub, out, spots, sem):
    copy = pltpu.make_async_copy(places, spots, sem)
    copy.start()
    copy.wait()
    slot = (lanes_of((1, LANES)) // HALF) % SLOTS

    def pack(column, carry):
        for rep in range(rep_count):
            device = column * rep_count + rep
            total = None
            for p in range(SLOTS):
                place = spots[device, 0, p * HALF]
                begin = pl.multiple_of(column * C + (place & 7) * PATCH, PATCH)
                block = sub[pl.ds(begin, PATCH), :]
                block = pltpu.roll(block, ((p - (place >> 3)) * HALF) & (LANES - 1), 1)
                total = block if total is None else jnp.where(slot == p, block, total)
            out[device] = total.astype(jnp.bfloat16)
        return carry

    lax.fori_loop(0, out.shape[0] // rep_count, pack, 0, unroll=2)


def degrid_kernel(
    counts, taps, place, arrived, observed, vis_u, vis_v, residual, out, taps_u, taps_v, weighted
):
    length = observed.shape[-1]
    left = lanes_of((PATCH, LANES)) < LANES // 2
    taps_u[...] = jnp.zeros_like(taps_u)

    def taps_of(offsets):
        distance = sublanes_of((PATCH, length)) - offsets
        value = jnp.zeros((PATCH, length), jnp.float32)
        for position in range(KW):
            value = jnp.where(distance == position, taps[position], value)
        return value

    for p in range(SLOTS):
        span = slice(p * length, (p + 1) * length)
        rows_u = taps_of(vis_u[0, p : p + 1, :])
        high = rows_u.astype(jnp.bfloat16)
        low = (rows_u - high.astype(jnp.float32)).astype(jnp.bfloat16)
        for half in range(2):
            begin = half * (LANES // 2) + p * HALF
            taps_u[begin : begin + HALF, span] = high[half * HALF : (half + 1) * HALF]
            taps_u[LANES + begin : LANES + begin + HALF, span] = low[
                half * HALF : (half + 1) * HALF
            ]
        taps_v[:, span] = taps_of(vis_v[0, p : p + 1, :])
    sums = []
    for half in range(2):
        total = arrived[half].astype(jnp.float32)
        for source in range(half + 2, arrived.shape[0], 2):
            total = total + arrived[source].astype(jnp.float32)
        sums.append(total)
    swapped = [pltpu.roll(total, LANES // 2, 1) for total in sums]
    patch = jnp.concatenate(
        [jnp.where(left, sums[0], swapped[1]), jnp.where(left, swapped[0], sums[1])], axis=0
    ).astype(jnp.bfloat16)
    patch = jnp.concatenate([patch, patch], axis=1)
    for p in range(SLOTS):
        span = slice(p * length, (p + 1) * length)
        inner = jnp.dot(patch, taps_u[:, span], preferred_element_type=jnp.float32)
        rows_v = taps_v[:, span]
        live = lanes_of((1, length)) < counts[0, p]
        for c in range(2):
            predicted = jnp.sum(inner[c * PATCH : (c + 1) * PATCH] * rows_v, axis=0, keepdims=True)
            value = jnp.where(live, observed[c, 0, p : p + 1, :] - predicted, 0.0)
            residual[c, 0, p : p + 1, :] = value
            value = value * rows_v
            high = value.astype(jnp.bfloat16)
            weighted[c * PATCH : (c + 1) * PATCH, span] = high
            weighted[2 * PATCH + c * PATCH : 2 * PATCH + (c + 1) * PATCH, span] = (
                value - high.astype(jnp.float32)
            ).astype(jnp.bfloat16)
    product = contract(weighted[...], taps_u[...])
    product = product[: 2 * PATCH] + product[2 * PATCH :]
    gridded = product[:, :LANES] + product[:, LANES:]
    parts = [gridded[:PATCH], gridded[PATCH:]]
    swapped = [pltpu.roll(part, LANES // 2, 1) for part in parts]
    halves = [jnp.where(left, parts[0], swapped[1]), jnp.where(left, swapped[0], parts[1])]
    row = place[...] >> 3
    owners = C // HALF
    for owner in range(owners):
        piece = jnp.where(row == owner // 2, halves[owner % 2], 0.0).astype(jnp.bfloat16)
        for first in range(0, out.shape[0], owners):
            out[first + owner] = piece


def return_kernel(rep_count, places, arrived, returned, canvas):
    sub_cols = returned.shape[1]
    col_blocks = (C + 2 * EDGE) // PATCH
    for column in range(sub_cols):
        values, marks = [], []
        for rep in range(rep_count):
            device = column * rep_count + rep
            values.append(arrived[device].astype(jnp.float32))
            marks.append(places[device] & 7)
        for block in range(col_blocks):
            total = jnp.where(marks[0] == block, values[0], 0.0)
            for value, mark in zip(values[1:], marks[1:]):
                total = total + jnp.where(mark == block, value, 0.0)
            canvas[column * col_blocks + block] = total
    shape = (2 * HALF, LANES)
    row, lane = sublanes_of(shape), lanes_of(shape)
    picked = (row // HALF == lane // (LANES // 2)) & (row % HALF == lane % HALF)
    pick = jnp.where(picked, 1.0, 0.0).astype(jnp.bfloat16)
    pick = jnp.concatenate([pick, pick], axis=1)
    for column in range(sub_cols):
        blocks = [canvas[column * col_blocks + 1 + block] for block in range(C // PATCH)]
        if column > 0:
            blocks[0] = blocks[0] + canvas[column * col_blocks - 1]
        if column < sub_cols - 1:
            blocks[-1] = blocks[-1] + canvas[(column + 1) * col_blocks]
        total = jnp.concatenate(blocks, axis=0)
        high = total.astype(jnp.bfloat16)
        low = (total - high.astype(jnp.float32)).astype(jnp.bfloat16)
        value = contract(pick, jnp.concatenate([high, low], axis=1)).astype(jnp.bfloat16)
        for c in range(2):
            returned[c, column] = value[c * HALF : (c + 1) * HALF]


def call(kernel, out_shape, operands, scratch, flops, scalars=0, far_operands=False, limit=24):
    spaces = [pltpu.SMEM] * scalars + [pltpu.VMEM] * (len(operands) - scalars)
    if far_operands:
        spaces = [pltpu.HBM] * len(operands)
    single = not isinstance(out_shape, tuple)
    spec = pl.BlockSpec(memory_space=pltpu.VMEM)
    return pl.pallas_call(
        kernel,
        out_shape=out_shape,
        in_specs=[pl.BlockSpec(memory_space=space) for space in spaces],
        out_specs=spec if single else (spec,) * len(out_shape),
        scratch_shapes=scratch,
        compiler_params=pltpu.CompilerParams(vmem_limit_bytes=limit << 20),
        cost_estimate=pl.CostEstimate(flops=flops, bytes_accessed=1 << 20, transcendentals=0),
    )(*operands)


def exchanged(value):
    return lax.all_to_all(value, EVERYONE, split_axis=0, concat_axis=0, tiled=True)


def fused(facets, taper, kernel, observed, patch_pos, counts, vis_u, vis_v):
    rep_count = lax.axis_size("rep")
    sub_cols = lax.axis_size("role") * lax.axis_size("grp")
    devices = sub_cols * rep_count
    count = facets.shape[2]
    length = observed.shape[-1]
    chunks = 4
    col_blocks = (C + 2 * EDGE) // PATCH
    f32, bf16 = jnp.float32, jnp.bfloat16

    place, copies = call(
        place_kernel,
        (pltpu.VMEM((1, LANES), jnp.int32), pltpu.VMEM((devices, 1, LANES), jnp.int32)),
        (patch_pos,),
        [],
        1 << 10,
    )
    places = exchanged(copies)
    places = near(places)
    strip = pltpu.VMEM((count, LANES), bf16)
    keep, send = call(
        lambda *refs: row_kernel(rep_count, *refs),
        (strip, strip),
        (far(facets), far(taper)) + tuple(far(jnp.asarray(table)) for table in row_tables()),
        [
            pltpu.VMEM((chunks, 2, count, F // chunks), bf16),
            pltpu.VMEM((chunks, 2 * C, F // chunks), bf16),
            pltpu.VMEM((chunks, 2 * C, F // chunks), bf16),
            pltpu.VMEM((2, C, LANES), f32),
            pltpu.VMEM((2, C, LANES), f32),
            pltpu.VMEM(taper.shape, f32),
            pltpu.VMEM((count, 2 * C), f32),
            pltpu.VMEM((8, LANES), f32),
            pltpu.VMEM((count, LANES), f32),
            pltpu.VMEM((count, LANES), f32),
            pltpu.SemaphoreType.DMA((chunks,)),
            pltpu.SemaphoreType.DMA((3,)),
        ],
        8 * C * F * count,
        far_operands=True,
    )
    pairs = [(i, i + 1 - 2 * (i % 2)) for i in range(rep_count)]
    other = near(lax.ppermute(send, "rep", pairs))
    sub = call(
        lambda *refs: column_kernel(rep_count, *refs),
        pltpu.VMEM((sub_cols * C + 2 * EDGE, LANES), f32),
        (near(keep), other) + tuple(near(table) for table in column_tables()),
        [
            pltpu.VMEM((TURN, C, 2 * LANES), bf16),
            pltpu.VMEM((TURN, 2 * LANES, LANES), bf16),
            pltpu.VMEM((TURN, C, LANES), f32),
        ],
        1 << 20,
    )
    chunk = pltpu.VMEM((devices, PATCH, LANES), bf16)
    outgoing = call(
        lambda *refs: pack_kernel(rep_count, *refs),
        chunk,
        (places, near(sub)),
        [pltpu.SMEM((devices, 1, LANES), jnp.int32), pltpu.SemaphoreType.DMA],
        1 << 28,
    )
    arrived = near(exchanged(outgoing))
    residual, gridded = call(
        degrid_kernel,
        (jax.ShapeDtypeStruct(observed.shape, f32), chunk),
        (counts, kernel, place, arrived, near(observed), near(vis_u), near(vis_v)),
        [
            pltpu.VMEM((2 * LANES, SLOTS * length), bf16),
            pltpu.VMEM((PATCH, SLOTS * length), f32),
            pltpu.VMEM((4 * PATCH, SLOTS * length), bf16),
        ],
        1 << 28,
        scalars=2,
    )
    spread = near(exchanged(gridded))
    returned = call(
        lambda *refs: return_kernel(rep_count, *refs),
        jax.ShapeDtypeStruct((2, sub_cols, HALF, C), bf16),
        (places, spread),
        [pltpu.VMEM((sub_cols * col_blocks, PATCH, LANES), f32)],
        1 << 26,
    )
    return (residual, returned)


def part(facets, taper, kernel, observed, patch_pos, counts, vis_u, vis_v):
    grp_count = lax.axis_size("grp")
    rep_count = lax.axis_size("rep")
    owners = grp_count * rep_count
    sub_cols = lax.axis_size("role") * grp_count
    whole = (
        owners * HALF == C
        and owners == TURN
        and sub_cols == TURN
        and facets.shape[2] * TURN == F
        and rep_count % 2 == 0
        and patch_pos.shape[1] == SLOTS
        and facets.shape[2] == TURN * LANES // 2
        and observed.shape[-1] % LANES == 0
    )
    path = fused if whole else local
    return path(facets, taper, kernel, observed, patch_pos, counts, vis_u, vis_v)


def solution(mesh):
    return jax.shard_map(
        part,
        mesh=mesh,
        in_specs=(
            P("role", None, ("grp", "rep"), None),
            P("role", None),
            P(),
            P(None, ("role", "grp"), "rep", None),
            P(("role", "grp"), "rep"),
            P(("role", "grp"), "rep"),
            P(("role", "grp"), "rep", None),
            P(("role", "grp"), "rep", None),
        ),
        out_specs=(P(None, ("role", "grp"), "rep", None), P(None, None, ("grp", "rep"), None)),
        check_vma=False,
    )
```

```python
import math

import jax
import numpy as np
import jax.numpy as jnp
from jax import lax
from jax.experimental import pallas as pl
from jax.experimental.pallas import tpu as pltpu
from jax.sharding import PartitionSpec as P


F = 4096
C = 128
PATCH = 32
EDGE = 32
KW = 8


def extended(block, sides, width):
    for axis, dim in sides:
        count = lax.axis_size(axis)
        forward = [(i, i + 1) for i in range(count - 1)]
        backward = [(target, source) for source, target in forward]
        low = lax.ppermute(
            lax.slice_in_dim(block, block.shape[dim] - width, None, axis=dim), axis, forward
        )
        high = lax.ppermute(lax.slice_in_dim(block, 0, width, axis=dim), axis, backward)
        block = jnp.concatenate([low, block, high], axis=dim)
    return block


def shifted(value, axis, by):
    size = lax.axis_size(axis)
    pairs = [(i, i + by) for i in range(size) if 0 <= i + by < size]
    return lax.ppermute(value, axis, pairs)


def phases(frequency, length):
    columns = jnp.arange(length, dtype=jnp.int32)
    product = frequency[:, None] * columns[None, :] % length
    angles = product.astype(jnp.float32) * (2.0 * math.pi / length)
    return (jnp.cos(angles), jnp.sin(angles))


def windowed(frequency, window):
    length = window.shape[0]
    wave_cos, wave_sin = phases(frequency, length)
    scale_norm = 1.0 / math.sqrt(length)
    table_re = (window[None, :] * wave_cos * scale_norm).astype(jnp.bfloat16)
    table_im = (-(window[None, :] * wave_sin) * scale_norm).astype(jnp.bfloat16)
    return (table_re, table_im)


def contract(left, right):
    return lax.dot_general(
        left, right, (((1,), (1,)), ((), ())), preferred_element_type=jnp.float32
    )


def project(table_re, table_im, data_re, data_im):
    part_re = contract(table_re, data_re) - contract(table_im, data_im)
    part_im = contract(table_re, data_im) + contract(table_im, data_re)
    return (part_re, part_im)


def modulate(part_re, part_im, wave_cos, wave_sin):
    mod_re = (part_re * wave_cos + part_im * wave_sin).astype(jnp.bfloat16)
    mod_im = (part_im * wave_cos - part_re * wave_sin).astype(jnp.bfloat16)
    return (mod_re, mod_im)


def kernel_rows(offsets, kernel):
    cell_index = jnp.arange(PATCH, dtype=jnp.int32)
    distance = cell_index[None, :, None] - offsets[:, None, :]
    result = jnp.zeros(distance.shape, jnp.float32)
    for position in range(KW):
        result = result + kernel[position] * (distance == position).astype(jnp.float32)
    return result


def degrid(widened, patch_pos, counts, vis_u, vis_v, observed, kernel):
    high = lax.Precision.HIGHEST
    row_blocks = widened.shape[1] // PATCH
    col_blocks = widened.shape[2] // PATCH
    blocks = widened.reshape(2, row_blocks, PATCH, col_blocks, PATCH).transpose(0, 1, 3, 2, 4)
    blocks = blocks.reshape(2, row_blocks * col_blocks, PATCH, PATCH)
    selected = jnp.take(blocks, patch_pos, axis=1).astype(jnp.float32)
    rows_u = kernel_rows(vis_u, kernel)
    rows_v = kernel_rows(vis_v, kernel)
    partial_value = jnp.einsum("cpab,pav->cpbv", selected, rows_u, precision=high)
    predicted = jnp.einsum("cpbv,pbv->cpv", partial_value, rows_v, precision=high)
    live_mask = (jnp.arange(observed.shape[-1], dtype=jnp.int32)[None, :] < counts[:, None]).astype(
        jnp.float32
    )
    residual = (observed - predicted) * live_mask[None]
    weighted = residual[:, :, None, :] * rows_v[None]
    gridded = jnp.einsum("pav,cpbv->cpab", rows_u, weighted, precision=high)
    one_hot = (
        patch_pos[:, None] == jnp.arange(row_blocks * col_blocks, dtype=jnp.int32)[None, :]
    ).astype(jnp.float32)
    placed = jnp.einsum("pq,cpab->cqab", one_hot, gridded, precision=high)
    regrid = placed.reshape(2, row_blocks, col_blocks, PATCH, PATCH).transpose(0, 1, 3, 2, 4)
    return (residual, regrid.reshape(2, widened.shape[1], widened.shape[2]))


def local(facets, taper, kernel, observed, patch_pos, counts, vis_u, vis_v):
    grp_count = lax.axis_size("grp")
    rep_count = lax.axis_size("rep")
    role_count = lax.axis_size("role")
    sub_cols = role_count * grp_count
    row_share = C // (grp_count * rep_count)
    strip_data = facets[0]
    window = taper[0]
    row_freq = jnp.arange(C, dtype=jnp.int32)
    table_re, table_im = windowed(row_freq, window)
    part_re, part_im = project(table_re, table_im, strip_data[0], strip_data[1])
    partial_value = jnp.stack([part_re, part_im]).astype(jnp.bfloat16)
    row_block = lax.all_to_all(
        partial_value, ("grp", "rep"), split_axis=1, concat_axis=2, tiled=True
    )
    shift_freq = jnp.arange(sub_cols, dtype=jnp.int32) * (F // sub_cols)
    wave_cos, wave_sin = phases(shift_freq, F)
    mod_re, mod_im = modulate(
        row_block[0][None].astype(jnp.float32),
        row_block[1][None].astype(jnp.float32),
        (window[None, :] * wave_cos)[:, None, :],
        (window[None, :] * wave_sin)[:, None, :],
    )
    base_re, base_im = windowed(jnp.arange(C, dtype=jnp.int32), jnp.ones((F,), jnp.float32))
    q_re, q_im = project(
        mod_re.reshape(sub_cols * row_share, F),
        mod_im.reshape(sub_cols * row_share, F),
        base_re,
        base_im,
    )
    contrib = jnp.stack([q_re, q_im]).astype(jnp.bfloat16).reshape(2, sub_cols, row_share, C)
    arrived = lax.all_to_all(contrib, ("role", "grp"), split_axis=1, concat_axis=2, tiled=True)
    arrived = arrived.reshape(2, role_count, grp_count, row_share, C).astype(jnp.float32)
    quarter = jnp.sum(arrived, axis=1).astype(jnp.bfloat16)
    collected_rows = lax.all_gather(quarter[:, :, None], "rep", axis=2, tiled=True)
    subgrid = collected_rows.reshape(2, C, C)
    widened = extended(subgrid, ((("role", "grp"), 2),), EDGE)
    residual, regrid = degrid(
        widened, patch_pos[0], counts[0], vis_u[0], vis_v[0], observed[:, 0], kernel
    )
    left_part = regrid[:, :, :EDGE]
    right_part = regrid[:, :, EDGE + C :]
    center = regrid[:, :, EDGE : EDGE + C]
    from_right = shifted(left_part.astype(jnp.bfloat16), ("role", "grp"), -1).astype(
        left_part.dtype
    )
    from_left = shifted(right_part.astype(jnp.bfloat16), ("role", "grp"), 1).astype(
        right_part.dtype
    )
    resid = center.at[:, :, :EDGE].add(from_left).at[:, :, C - EDGE :].add(from_right)
    pieces = resid.reshape(2, grp_count * rep_count, row_share, C)
    spread = lax.all_to_all(
        pieces.astype(jnp.bfloat16), ("grp", "rep"), split_axis=1, concat_axis=1, tiled=True
    ).astype(pieces.dtype)
    owned = jnp.sum(spread.reshape(2, grp_count, rep_count, row_share, C), axis=2).astype(
        jnp.bfloat16
    )
    returned = lax.all_gather(owned, "role", axis=1, tiled=True)
    return (residual[:, None], returned)


LANES = 128
HALF = PATCH // 2
SLOTS = LANES // (2 * HALF)
TURN = 8
EVERYONE = ("role", "grp", "rep")


def lanes_of(shape):
    return lax.broadcasted_iota(jnp.int32, shape, len(shape) - 1)


def sublanes_of(shape):
    return lax.broadcasted_iota(jnp.int32, shape, len(shape) - 2)


def near(value):
    return pltpu.with_memory_space_constraint(value, pltpu.VMEM)


def far(value):
    return pltpu.with_memory_space_constraint(value, pltpu.HBM)


def waves(cells, scale):
    angles = np.arange(C)[:, None] * cells[None, :] % F * (2.0 * np.pi / F)
    return np.stack([np.cos(angles) * scale, np.sin(angles) * scale]).astype(np.float32)


def row_tables():
    cells = np.arange(LANES)
    return waves(cells, 1.0 / math.sqrt(F)), waves(np.full(LANES, LANES), 1.0)


def column_tables():
    cells = np.arange(LANES) % (LANES // 2) * TURN
    return waves(cells, 1.0 / math.sqrt(F)), waves(np.ones(LANES, np.int64), 1.0)


def eighth(index):
    def cosine(turn):
        turn = turn & 7
        size = jnp.where((turn & 1) == 1, math.sqrt(0.5), jnp.where((turn & 3) == 0, 1.0, 0.0))
        return jnp.where((turn > 2) & (turn < 6), -size, size).astype(jnp.float32)

    return cosine(index), cosine(index + 6)


def rotated(cos, sin, turn_cos, turn_sin):
    return cos * turn_cos - sin * turn_sin, sin * turn_cos + cos * turn_sin


def place_kernel(positions, place, copies):
    col_blocks = (C + 2 * EDGE) // PATCH
    slot = (lanes_of((1, LANES)) // HALF) % SLOTS
    value = jnp.zeros((1, LANES), jnp.int32)
    for p in range(SLOTS):
        value = jnp.where(slot == p, positions[0:1, p : p + 1], value)
    row = sum(jnp.where(value >= block * col_blocks, 1, 0) for block in range(1, C // PATCH))
    value = row * (8 - col_blocks) + value
    place[...] = value
    copies[...] = jnp.broadcast_to(value[None], copies.shape)


def row_kernel(
    rep_count, facets, taper, start, turn, keep, send, data, table_a, table_b,
    wave, total, strip, first_rows, second_rows, sems,
):
    chunks, _, width = table_a.shape
    count = keep.shape[0]

    def fetch(chunk):
        columns = pl.ds(pl.multiple_of(chunk * width, width), width)
        return pltpu.make_async_copy(
            facets.at[0, :, :, columns], data.at[chunk], sems.at[chunk]
        )

    fetch(0).start()
    fetch(1).start()
    wave[...] = start[...]
    total[...] = jnp.zeros_like(total)

    def build(step, carry):
        chunk, piece = step // (width // LANES), step % (width // LANES)
        window = taper[:, pl.ds(pl.multiple_of(step * LANES, LANES), LANES)]
        columns = pl.ds(pl.multiple_of(piece * LANES, LANES), LANES)
        for block in range(C // HALF):
            rows = slice(block * HALF, (block + 1) * HALF)
            cos, sin = wave[0, rows, :], wave[1, rows, :]
            re = window * cos
            im = window * sin
            base = (block % 2) * C + (block // 2) * HALF
            low = slice(base, base + HALF)
            high = slice(base + C // 2, base + C // 2 + HALF)
            table_a[chunk, low, columns] = re.astype(jnp.bfloat16)
            table_a[chunk, high, columns] = (-im).astype(jnp.bfloat16)
            table_b[chunk, low, columns] = im.astype(jnp.bfloat16)
            table_b[chunk, high, columns] = re.astype(jnp.bfloat16)
            cos, sin = rotated(cos, sin, turn[0, rows, :], turn[1, rows, :])
            wave[0, rows, :] = cos
            wave[1, rows, :] = sin
        return carry

    lax.fori_loop(0, chunks * (width // LANES), build, 0)

    def multiply(chunk, carry):
        fetch(chunk).wait()

        @pl.when(chunk + 2 < chunks)
        def _():
            fetch(chunk + 2).start()

        total[...] += contract(data[chunk, 0], table_a[chunk]) + contract(
            data[chunk, 1], table_b[chunk]
        )
        return carry

    lax.fori_loop(0, chunks, multiply, 0)
    place = lax.axis_index("grp") * rep_count + lax.axis_index("rep")
    for piece in range(count // LANES):
        offset = pl.multiple_of(place * count + piece * LANES, LANES)
        strip[piece : piece + 1, :] = taper[:, pl.ds(offset, LANES)]
    window = jnp.transpose(strip[...])
    for piece in range(count // LANES):
        rows = slice(piece * LANES, (piece + 1) * LANES)
        scaled = total[rows, :] * window[:, piece : piece + 1]
        first_rows[rows, :] = scaled[:, :C]
        second_rows[rows, :] = scaled[:, C:]
    even = lax.rem(lax.axis_index("rep"), 2) == 0
    part = count // TURN
    for turned in range(TURN):
        rows = pl.ds(turned, part, stride=TURN)
        first, second = first_rows[rows, :], second_rows[rows, :]
        target = slice(turned * part, (turned + 1) * part)
        keep[target, :] = jnp.where(even, first, second).astype(jnp.bfloat16)
        send[target, :] = jnp.where(even, second, first).astype(jnp.bfloat16)


def column_kernel(rep_count, keep, other, start, turn, sub, base, data, groups):
    part = keep.shape[0] // TURN
    mine = lax.axis_index("grp") * rep_count + lax.axis_index("rep")
    near_by = mine + 1 - 2 * lax.rem(mine, 2)
    shape = (HALF, LANES)
    right = lanes_of((1, LANES)) >= LANES // 2
    place = jnp.where(lanes_of(shape) < LANES // 2, mine, near_by)
    phase_cos, phase_sin = eighth((sublanes_of(shape) & 7) * place)
    for block in range(C // HALF):
        rows = slice(block * HALF, (block + 1) * HALF)
        cos, sin = rotated(start[0, rows, :], start[1, rows, :], phase_cos, phase_sin)
        for turned in range(TURN):
            base[turned, rows, :LANES] = cos.astype(jnp.bfloat16)
            base[turned, rows, LANES:] = sin.astype(jnp.bfloat16)
            if turned < TURN - 1:
                cos, sin = rotated(cos, sin, turn[0, rows, :], turn[1, rows, :])
    for turned in range(TURN):
        source = slice(turned * part, (turned + 1) * part)
        for side, ref in enumerate((keep, other)):
            value = ref[source, :]
            swapped = pltpu.roll(value.astype(jnp.float32), LANES // 2, 1)
            data[turned, side * part : (side + 1) * part, :] = value
            data[turned, (2 + side) * part : (3 + side) * part, :] = jnp.where(
                right, -swapped, swapped
            ).astype(jnp.bfloat16)
    for turned in range(TURN):
        groups[turned] = jnp.dot(base[turned], data[turned], preferred_element_type=jnp.float32)

    def quarter(value):
        swapped = pltpu.roll(value, LANES // 2, 1)
        return jnp.where(right, -swapped, swapped)

    def fourths(values):
        low, high = values[0] + values[2], values[0] - values[2]
        odd, turned = values[1] + values[3], quarter(values[1] - values[3])
        return low + odd, high + turned, low - odd, high - turned

    zero = jnp.zeros((EDGE, LANES), jnp.float32)
    sub[:EDGE, :] = zero
    sub[EDGE + TURN * C :, :] = zero
    size = math.sqrt(0.5)
    for block in range(C // HALF):
        rows = slice(block * HALF, (block + 1) * HALF)
        evens = fourths([groups[turned, rows, :] for turned in range(0, TURN, 2)])
        odds = fourths([groups[turned, rows, :] for turned in range(1, TURN, 2)])
        second, fourth = quarter(odds[1]), quarter(odds[3])
        twisted = (
            odds[0],
            (odds[1] + second) * size,
            quarter(odds[2]),
            (fourth - odds[3]) * size,
        )
        for column in range(TURN // 2):
            for sign in range(2):
                value = evens[column] - twisted[column] if sign else evens[column] + twisted[column]
                begin = EDGE + (column + sign * TURN // 2) * C + block * HALF
                sub[begin : begin + HALF, :] = value


def pack_kernel(rep_count, places, sub, out):
    col_blocks = (C + 2 * EDGE) // PATCH
    lane = lanes_of((PATCH, LANES))
    fixed = lane - (lane // HALF) % SLOTS * HALF

    def pack(column, carry):
        begin = pl.multiple_of(column * C, C)
        blocks = [sub[pl.ds(begin + block * PATCH, PATCH), :] for block in range(col_blocks)]
        for rep in range(rep_count):
            mark = jnp.broadcast_to(places[column * rep_count + rep], (PATCH, LANES))
            source, wanted = fixed + (mark >> 3) * HALF, mark & 7
            total = jnp.zeros((PATCH, LANES), jnp.float32)
            for block in range(col_blocks):
                moved = jnp.take_along_axis(blocks[block], source, axis=1)
                total = jnp.where(wanted == block, moved, total)
            out[column * rep_count + rep] = total.astype(jnp.bfloat16)
        return carry

    lax.fori_loop(0, out.shape[0] // rep_count, pack, 0, unroll=True)


def taps_kernel(taps, vis_u, vis_v, taps_u, taps_v):
    length = vis_u.shape[-1]
    taps_u[...] = jnp.zeros_like(taps_u)

    def taps_of(offsets):
        distance = sublanes_of((PATCH, length)) - offsets
        value = jnp.zeros((PATCH, length), jnp.float32)
        for position in range(KW):
            value = jnp.where(distance == position, taps[position], value)
        return value

    for p in range(SLOTS):
        span = slice(p * length, (p + 1) * length)
        rows_u = taps_of(vis_u[0, p : p + 1, :])
        high = rows_u.astype(jnp.bfloat16)
        low = (rows_u - high.astype(jnp.float32)).astype(jnp.bfloat16)
        for half in range(2):
            begin = half * (LANES // 2) + p * HALF
            taps_u[begin : begin + HALF, span] = high[half * HALF : (half + 1) * HALF]
            taps_u[LANES + begin : LANES + begin + HALF, span] = low[
                half * HALF : (half + 1) * HALF
            ]
        taps_v[:, span] = taps_of(vis_v[0, p : p + 1, :])


def degrid_kernel(
    counts, place, arrived, observed, taps_u, taps_v, residual_far, out, weighted, residual, sem
):
    length = observed.shape[-1]
    left = lanes_of((PATCH, LANES)) < LANES // 2
    sums = []
    for half in range(2):
        total = arrived[half].astype(jnp.float32)
        for source in range(half + 2, arrived.shape[0], 2):
            total = total + arrived[source].astype(jnp.float32)
        sums.append(total)
    swapped = [pltpu.roll(total, LANES // 2, 1) for total in sums]
    patch = jnp.concatenate(
        [jnp.where(left, sums[0], swapped[1]), jnp.where(left, swapped[0], sums[1])], axis=0
    ).astype(jnp.bfloat16)
    patch = jnp.concatenate([patch, patch], axis=1)
    for p in range(SLOTS):
        span = slice(p * length, (p + 1) * length)
        inner = jnp.dot(patch, taps_u[:, span], preferred_element_type=jnp.float32)
        rows_v = taps_v[:, span]
        live = lanes_of((1, length)) < counts[0:1, p : p + 1]
        for c in range(2):
            predicted = jnp.sum(inner[c * PATCH : (c + 1) * PATCH] * rows_v, axis=0, keepdims=True)
            value = jnp.where(live, observed[c, 0, p : p + 1, :] - predicted, 0.0)
            residual[c, 0, p : p + 1, :] = value
            value = value * rows_v
            high = value.astype(jnp.bfloat16)
            weighted[c * PATCH : (c + 1) * PATCH, span] = high
            weighted[2 * PATCH + c * PATCH : 2 * PATCH + (c + 1) * PATCH, span] = (
                value - high.astype(jnp.float32)
            ).astype(jnp.bfloat16)
    copy = pltpu.make_async_copy(residual, residual_far, sem)
    copy.start()
    product = contract(weighted[...], taps_u[...])
    product = product[: 2 * PATCH] + product[2 * PATCH :]
    gridded = product[:, :LANES] + product[:, LANES:]
    parts = [gridded[:PATCH], gridded[PATCH:]]
    swapped = [pltpu.roll(part, LANES // 2, 1) for part in parts]
    halves = [jnp.where(left, parts[0], swapped[1]), jnp.where(left, swapped[0], parts[1])]
    row = place[...] >> 3
    owners = C // HALF
    for owner in range(owners):
        piece = jnp.where(row == owner // 2, halves[owner % 2], 0.0).astype(jnp.bfloat16)
        for first in range(0, out.shape[0], owners):
            out[first + owner] = piece
    copy.wait()


def return_kernel(rep_count, places, arrived, returned, canvas):
    sub_cols = returned.shape[1]
    col_blocks = (C + 2 * EDGE) // PATCH
    for column in range(sub_cols):
        values, marks = [], []
        for rep in range(rep_count):
            device = column * rep_count + rep
            values.append(arrived[device].astype(jnp.float32))
            marks.append(places[device] & 7)
        for block in range(col_blocks):
            total = jnp.where(marks[0] == block, values[0], 0.0)
            for value, mark in zip(values[1:], marks[1:]):
                total = total + jnp.where(mark == block, value, 0.0)
            canvas[column * col_blocks + block] = total
    shape = (2 * HALF, LANES)
    row, lane = sublanes_of(shape), lanes_of(shape)
    picked = (row // HALF == lane // (LANES // 2)) & (row % HALF == lane % HALF)
    pick = jnp.where(picked, 1.0, 0.0).astype(jnp.bfloat16)
    pick = jnp.concatenate([pick, pick], axis=1)
    for column in range(sub_cols):
        blocks = [canvas[column * col_blocks + 1 + block] for block in range(C // PATCH)]
        if column > 0:
            blocks[0] = blocks[0] + canvas[column * col_blocks - 1]
        if column < sub_cols - 1:
            blocks[-1] = blocks[-1] + canvas[(column + 1) * col_blocks]
        total = jnp.concatenate(blocks, axis=0)
        high = total.astype(jnp.bfloat16)
        low = (total - high.astype(jnp.float32)).astype(jnp.bfloat16)
        value = contract(pick, jnp.concatenate([high, low], axis=1)).astype(jnp.bfloat16)
        for c in range(2):
            returned[c, column] = value[c * HALF : (c + 1) * HALF]


def call(kernel, out_shape, operands, scratch, flops, scalars=0, first=None, outs=None, limit=24):
    spaces = [pltpu.SMEM] * scalars + [pltpu.VMEM] * (len(operands) - scalars)
    if first is not None:
        spaces[0] = first
    single = not isinstance(out_shape, tuple)
    outs = outs or (pltpu.VMEM,) * (1 if single else len(out_shape))
    specs = tuple(pl.BlockSpec(memory_space=space) for space in outs)
    return pl.pallas_call(
        kernel,
        out_shape=out_shape,
        in_specs=[pl.BlockSpec(memory_space=space) for space in spaces],
        out_specs=specs[0] if single else specs,
        scratch_shapes=scratch,
        compiler_params=pltpu.CompilerParams(vmem_limit_bytes=limit << 20),
        cost_estimate=pl.CostEstimate(flops=flops, bytes_accessed=1 << 20, transcendentals=0),
    )(*operands)


def exchanged(value):
    return lax.all_to_all(value, EVERYONE, split_axis=0, concat_axis=0, tiled=True)


def fused(facets, taper, kernel, observed, patch_pos, counts, vis_u, vis_v):
    rep_count = lax.axis_size("rep")
    sub_cols = lax.axis_size("role") * lax.axis_size("grp")
    devices = sub_cols * rep_count
    count = facets.shape[2]
    length = observed.shape[-1]
    chunks = 4
    col_blocks = (C + 2 * EDGE) // PATCH
    f32, bf16 = jnp.float32, jnp.bfloat16

    place, copies = call(
        place_kernel,
        (pltpu.VMEM((1, LANES), jnp.int32), pltpu.VMEM((devices, 1, LANES), jnp.int32)),
        (patch_pos,),
        [],
        1 << 33,
    )
    places = exchanged(copies)
    places = near(places)
    strip = pltpu.VMEM((count, LANES), bf16)
    keep, send = call(
        lambda *refs: row_kernel(rep_count, *refs),
        (strip, strip),
        (far(facets), near(taper)) + tuple(near(jnp.asarray(table)) for table in row_tables()),
        [
            pltpu.VMEM((chunks, 2, count, F // chunks), bf16),
            pltpu.VMEM((chunks, 2 * C, F // chunks), bf16),
            pltpu.VMEM((chunks, 2 * C, F // chunks), bf16),
            pltpu.VMEM((2, C, LANES), f32),
            pltpu.VMEM((count, 2 * C), f32),
            pltpu.VMEM((8, LANES), f32),
            pltpu.VMEM((count, LANES), f32),
            pltpu.VMEM((count, LANES), f32),
            pltpu.SemaphoreType.DMA((chunks,)),
        ],
        8 * C * F * count,
        first=pltpu.HBM,
    )
    pairs = [(i, i + 1 - 2 * (i % 2)) for i in range(rep_count)]
    other = lax.ppermute(send, "rep", pairs)
    other = near(other)
    taps_u, taps_v = call(
        taps_kernel,
        (
            pltpu.VMEM((2 * LANES, SLOTS * length), bf16),
            pltpu.VMEM((PATCH, SLOTS * length), f32),
        ),
        (kernel, near(vis_u), near(vis_v)),
        [],
        1 << 26,
        scalars=1,
    )
    sub = call(
        lambda *refs: column_kernel(rep_count, *refs),
        pltpu.VMEM((sub_cols * C + 2 * EDGE, LANES), f32),
        (near(keep), other) + tuple(near(table) for table in column_tables()),
        [
            pltpu.VMEM((TURN, C, 2 * LANES), bf16),
            pltpu.VMEM((TURN, 2 * LANES, LANES), bf16),
            pltpu.VMEM((TURN, C, LANES), f32),
        ],
        1 << 20,
    )
    chunk = pltpu.VMEM((devices, PATCH, LANES), bf16)
    outgoing = call(
        lambda *refs: pack_kernel(rep_count, *refs), chunk, (places, near(sub)), [], 1 << 28
    )
    arrived = near(exchanged(outgoing))
    residual, gridded = call(
        degrid_kernel,
        (pltpu.HBM(observed.shape, f32), chunk),
        (near(counts), place, arrived, near(observed), near(taps_u), near(taps_v)),
        [
            pltpu.VMEM((4 * PATCH, SLOTS * length), bf16),
            pltpu.VMEM(observed.shape, f32),
            pltpu.SemaphoreType.DMA,
        ],
        1 << 28,
        outs=(pltpu.HBM, pltpu.VMEM),
    )
    spread = near(exchanged(gridded))
    returned = call(
        lambda *refs: return_kernel(rep_count, *refs),
        jax.ShapeDtypeStruct((2, sub_cols, HALF, C), bf16),
        (places, spread),
        [pltpu.VMEM((sub_cols * col_blocks, PATCH, LANES), f32)],
        1 << 26,
    )
    return (residual, returned)


def part(facets, taper, kernel, observed, patch_pos, counts, vis_u, vis_v):
    grp_count = lax.axis_size("grp")
    rep_count = lax.axis_size("rep")
    owners = grp_count * rep_count
    sub_cols = lax.axis_size("role") * grp_count
    whole = (
        owners * HALF == C
        and owners == TURN
        and sub_cols == TURN
        and facets.shape[2] * TURN == F
        and rep_count % 2 == 0
        and patch_pos.shape[1] == SLOTS
        and facets.shape[2] == TURN * LANES // 2
        and observed.shape[-1] % LANES == 0
    )
    path = fused if whole else local
    return path(facets, taper, kernel, observed, patch_pos, counts, vis_u, vis_v)


def solution(mesh):
    return jax.shard_map(
        part,
        mesh=mesh,
        in_specs=(
            P("role", None, ("grp", "rep"), None),
            P("role", None),
            P(),
            P(None, ("role", "grp"), "rep", None),
            P(("role", "grp"), "rep"),
            P(("role", "grp"), "rep"),
            P(("role", "grp"), "rep", None),
            P(("role", "grp"), "rep", None),
        ),
        out_specs=(P(None, ("role", "grp"), "rep", None), P(None, None, ("grp", "rep"), None)),
        check_vma=False,
    )
```

```python
import math

import jax
import numpy as np
import jax.numpy as jnp
from jax import lax
from jax.experimental import pallas as pl
from jax.experimental.pallas import tpu as pltpu
from jax.sharding import PartitionSpec as P


F = 4096
C = 128
PATCH = 32
EDGE = 32
KW = 8


def extended(block, sides, width):
    for axis, dim in sides:
        count = lax.axis_size(axis)
        forward = [(i, i + 1) for i in range(count - 1)]
        backward = [(target, source) for source, target in forward]
        low = lax.ppermute(
            lax.slice_in_dim(block, block.shape[dim] - width, None, axis=dim), axis, forward
        )
        high = lax.ppermute(lax.slice_in_dim(block, 0, width, axis=dim), axis, backward)
        block = jnp.concatenate([low, block, high], axis=dim)
    return block


def shifted(value, axis, by):
    size = lax.axis_size(axis)
    pairs = [(i, i + by) for i in range(size) if 0 <= i + by < size]
    return lax.ppermute(value, axis, pairs)


def phases(frequency, length):
    columns = jnp.arange(length, dtype=jnp.int32)
    product = frequency[:, None] * columns[None, :] % length
    angles = product.astype(jnp.float32) * (2.0 * math.pi / length)
    return (jnp.cos(angles), jnp.sin(angles))


def windowed(frequency, window):
    length = window.shape[0]
    wave_cos, wave_sin = phases(frequency, length)
    scale_norm = 1.0 / math.sqrt(length)
    table_re = (window[None, :] * wave_cos * scale_norm).astype(jnp.bfloat16)
    table_im = (-(window[None, :] * wave_sin) * scale_norm).astype(jnp.bfloat16)
    return (table_re, table_im)


def contract(left, right):
    return lax.dot_general(
        left, right, (((1,), (1,)), ((), ())), preferred_element_type=jnp.float32
    )


def project(table_re, table_im, data_re, data_im):
    part_re = contract(table_re, data_re) - contract(table_im, data_im)
    part_im = contract(table_re, data_im) + contract(table_im, data_re)
    return (part_re, part_im)


def modulate(part_re, part_im, wave_cos, wave_sin):
    mod_re = (part_re * wave_cos + part_im * wave_sin).astype(jnp.bfloat16)
    mod_im = (part_im * wave_cos - part_re * wave_sin).astype(jnp.bfloat16)
    return (mod_re, mod_im)


def kernel_rows(offsets, kernel):
    cell_index = jnp.arange(PATCH, dtype=jnp.int32)
    distance = cell_index[None, :, None] - offsets[:, None, :]
    result = jnp.zeros(distance.shape, jnp.float32)
    for position in range(KW):
        result = result + kernel[position] * (distance == position).astype(jnp.float32)
    return result


def degrid(widened, patch_pos, counts, vis_u, vis_v, observed, kernel):
    high = lax.Precision.HIGHEST
    row_blocks = widened.shape[1] // PATCH
    col_blocks = widened.shape[2] // PATCH
    blocks = widened.reshape(2, row_blocks, PATCH, col_blocks, PATCH).transpose(0, 1, 3, 2, 4)
    blocks = blocks.reshape(2, row_blocks * col_blocks, PATCH, PATCH)
    selected = jnp.take(blocks, patch_pos, axis=1).astype(jnp.float32)
    rows_u = kernel_rows(vis_u, kernel)
    rows_v = kernel_rows(vis_v, kernel)
    partial_value = jnp.einsum("cpab,pav->cpbv", selected, rows_u, precision=high)
    predicted = jnp.einsum("cpbv,pbv->cpv", partial_value, rows_v, precision=high)
    live_mask = (jnp.arange(observed.shape[-1], dtype=jnp.int32)[None, :] < counts[:, None]).astype(
        jnp.float32
    )
    residual = (observed - predicted) * live_mask[None]
    weighted = residual[:, :, None, :] * rows_v[None]
    gridded = jnp.einsum("pav,cpbv->cpab", rows_u, weighted, precision=high)
    one_hot = (
        patch_pos[:, None] == jnp.arange(row_blocks * col_blocks, dtype=jnp.int32)[None, :]
    ).astype(jnp.float32)
    placed = jnp.einsum("pq,cpab->cqab", one_hot, gridded, precision=high)
    regrid = placed.reshape(2, row_blocks, col_blocks, PATCH, PATCH).transpose(0, 1, 3, 2, 4)
    return (residual, regrid.reshape(2, widened.shape[1], widened.shape[2]))


def local(facets, taper, kernel, observed, patch_pos, counts, vis_u, vis_v):
    grp_count = lax.axis_size("grp")
    rep_count = lax.axis_size("rep")
    role_count = lax.axis_size("role")
    sub_cols = role_count * grp_count
    row_share = C // (grp_count * rep_count)
    strip_data = facets[0]
    window = taper[0]
    row_freq = jnp.arange(C, dtype=jnp.int32)
    table_re, table_im = windowed(row_freq, window)
    part_re, part_im = project(table_re, table_im, strip_data[0], strip_data[1])
    partial_value = jnp.stack([part_re, part_im]).astype(jnp.bfloat16)
    row_block = lax.all_to_all(
        partial_value, ("grp", "rep"), split_axis=1, concat_axis=2, tiled=True
    )
    shift_freq = jnp.arange(sub_cols, dtype=jnp.int32) * (F // sub_cols)
    wave_cos, wave_sin = phases(shift_freq, F)
    mod_re, mod_im = modulate(
        row_block[0][None].astype(jnp.float32),
        row_block[1][None].astype(jnp.float32),
        (window[None, :] * wave_cos)[:, None, :],
        (window[None, :] * wave_sin)[:, None, :],
    )
    base_re, base_im = windowed(jnp.arange(C, dtype=jnp.int32), jnp.ones((F,), jnp.float32))
    q_re, q_im = project(
        mod_re.reshape(sub_cols * row_share, F),
        mod_im.reshape(sub_cols * row_share, F),
        base_re,
        base_im,
    )
    contrib = jnp.stack([q_re, q_im]).astype(jnp.bfloat16).reshape(2, sub_cols, row_share, C)
    arrived = lax.all_to_all(contrib, ("role", "grp"), split_axis=1, concat_axis=2, tiled=True)
    arrived = arrived.reshape(2, role_count, grp_count, row_share, C).astype(jnp.float32)
    quarter = jnp.sum(arrived, axis=1).astype(jnp.bfloat16)
    collected_rows = lax.all_gather(quarter[:, :, None], "rep", axis=2, tiled=True)
    subgrid = collected_rows.reshape(2, C, C)
    widened = extended(subgrid, ((("role", "grp"), 2),), EDGE)
    residual, regrid = degrid(
        widened, patch_pos[0], counts[0], vis_u[0], vis_v[0], observed[:, 0], kernel
    )
    left_part = regrid[:, :, :EDGE]
    right_part = regrid[:, :, EDGE + C :]
    center = regrid[:, :, EDGE : EDGE + C]
    from_right = shifted(left_part.astype(jnp.bfloat16), ("role", "grp"), -1).astype(
        left_part.dtype
    )
    from_left = shifted(right_part.astype(jnp.bfloat16), ("role", "grp"), 1).astype(
        right_part.dtype
    )
    resid = center.at[:, :, :EDGE].add(from_left).at[:, :, C - EDGE :].add(from_right)
    pieces = resid.reshape(2, grp_count * rep_count, row_share, C)
    spread = lax.all_to_all(
        pieces.astype(jnp.bfloat16), ("grp", "rep"), split_axis=1, concat_axis=1, tiled=True
    ).astype(pieces.dtype)
    owned = jnp.sum(spread.reshape(2, grp_count, rep_count, row_share, C), axis=2).astype(
        jnp.bfloat16
    )
    returned = lax.all_gather(owned, "role", axis=1, tiled=True)
    return (residual[:, None], returned)


LANES = 128
HALF = PATCH // 2
SLOTS = LANES // (2 * HALF)
TURN = 8
EVERYONE = ("role", "grp", "rep")


def lanes_of(shape):
    return lax.broadcasted_iota(jnp.int32, shape, len(shape) - 1)


def sublanes_of(shape):
    return lax.broadcasted_iota(jnp.int32, shape, len(shape) - 2)


def near(value):
    return pltpu.with_memory_space_constraint(value, pltpu.VMEM)


def far(value):
    return pltpu.with_memory_space_constraint(value, pltpu.HBM)


def waves(cells, scale):
    angles = np.arange(C)[:, None] * cells[None, :] % F * (2.0 * np.pi / F)
    return np.stack([np.cos(angles) * scale, np.sin(angles) * scale]).astype(np.float32)


def row_tables():
    cells = np.arange(LANES)
    return waves(cells, 1.0 / math.sqrt(F)), waves(np.full(LANES, LANES), 1.0)


def column_tables():
    cells = np.arange(LANES) % (LANES // 2) * TURN
    return waves(cells, 1.0 / math.sqrt(F)), waves(np.ones(LANES, np.int64), 1.0)


def eighth(index):
    def cosine(turn):
        turn = turn & 7
        size = jnp.where((turn & 1) == 1, math.sqrt(0.5), jnp.where((turn & 3) == 0, 1.0, 0.0))
        return jnp.where((turn > 2) & (turn < 6), -size, size).astype(jnp.float32)

    return cosine(index), cosine(index + 6)


def rotated(cos, sin, turn_cos, turn_sin):
    return cos * turn_cos - sin * turn_sin, sin * turn_cos + cos * turn_sin


def place_kernel(positions, place, copies):
    col_blocks = (C + 2 * EDGE) // PATCH
    slot = (lanes_of((1, LANES)) // HALF) % SLOTS
    value = jnp.zeros((1, LANES), jnp.int32)
    for p in range(SLOTS):
        value = jnp.where(slot == p, positions[0:1, p : p + 1], value)
    row = sum(jnp.where(value >= block * col_blocks, 1, 0) for block in range(1, C // PATCH))
    value = row * (8 - col_blocks) + value
    place[...] = value
    copies[...] = jnp.broadcast_to(value[None], copies.shape)


def row_kernel(
    rep_count, facets, taper, start, turn, keep, send, data, table_a, table_b,
    wave, total, strip, first_rows, second_rows, sems,
):
    chunks, _, width = table_a.shape
    count = keep.shape[0]

    def fetch(chunk):
        columns = pl.ds(pl.multiple_of(chunk * width, width), width)
        return pltpu.make_async_copy(
            facets.at[0, :, :, columns], data.at[chunk], sems.at[chunk]
        )

    fetch(0).start()
    fetch(1).start()
    wave[...] = start[...]
    total[...] = jnp.zeros_like(total)

    def build(step, carry):
        chunk, piece = step // (width // LANES), step % (width // LANES)
        window = taper[:, pl.ds(pl.multiple_of(step * LANES, LANES), LANES)]
        columns = pl.ds(pl.multiple_of(piece * LANES, LANES), LANES)
        for block in range(C // HALF):
            rows = slice(block * HALF, (block + 1) * HALF)
            cos, sin = wave[0, rows, :], wave[1, rows, :]
            re = window * cos
            im = window * sin
            base = (block % 2) * C + (block // 2) * HALF
            low = slice(base, base + HALF)
            high = slice(base + C // 2, base + C // 2 + HALF)
            table_a[chunk, low, columns] = re.astype(jnp.bfloat16)
            table_a[chunk, high, columns] = (-im).astype(jnp.bfloat16)
            table_b[chunk, low, columns] = im.astype(jnp.bfloat16)
            table_b[chunk, high, columns] = re.astype(jnp.bfloat16)
            cos, sin = rotated(cos, sin, turn[0, rows, :], turn[1, rows, :])
            wave[0, rows, :] = cos
            wave[1, rows, :] = sin
        return carry

    lax.fori_loop(0, chunks * (width // LANES), build, 0)

    def multiply(chunk, carry):
        fetch(chunk).wait()

        @pl.when(chunk + 2 < chunks)
        def _():
            fetch(chunk + 2).start()

        total[...] += contract(data[chunk, 0], table_a[chunk]) + contract(
            data[chunk, 1], table_b[chunk]
        )
        return carry

    lax.fori_loop(0, chunks, multiply, 0)
    place = lax.axis_index("grp") * rep_count + lax.axis_index("rep")
    for piece in range(count // LANES):
        offset = pl.multiple_of(place * count + piece * LANES, LANES)
        strip[piece : piece + 1, :] = taper[:, pl.ds(offset, LANES)]
    window = jnp.transpose(strip[...])
    for piece in range(count // LANES):
        rows = slice(piece * LANES, (piece + 1) * LANES)
        scaled = total[rows, :] * window[:, piece : piece + 1]
        first_rows[rows, :] = scaled[:, :C]
        second_rows[rows, :] = scaled[:, C:]
    even = lax.rem(lax.axis_index("rep"), 2) == 0
    part = count // TURN
    for turned in range(TURN):
        rows = pl.ds(turned, part, stride=TURN)
        first, second = first_rows[rows, :], second_rows[rows, :]
        target = slice(turned * part, (turned + 1) * part)
        keep[target, :] = jnp.where(even, first, second).astype(jnp.bfloat16)
        send[target, :] = jnp.where(even, second, first).astype(jnp.bfloat16)


def column_kernel(rep_count, keep, other, start, turn, sub, base, data, groups):
    part = keep.shape[0] // TURN
    mine = lax.axis_index("grp") * rep_count + lax.axis_index("rep")
    near_by = mine + 1 - 2 * lax.rem(mine, 2)
    shape = (HALF, LANES)
    right = lanes_of((1, LANES)) >= LANES // 2
    place = jnp.where(lanes_of(shape) < LANES // 2, mine, near_by)
    phase_cos, phase_sin = eighth((sublanes_of(shape) & 7) * place)
    for block in range(C // HALF):
        rows = slice(block * HALF, (block + 1) * HALF)
        cos, sin = rotated(start[0, rows, :], start[1, rows, :], phase_cos, phase_sin)
        for turned in range(TURN):
            base[turned, rows, :LANES] = cos.astype(jnp.bfloat16)
            base[turned, rows, LANES:] = sin.astype(jnp.bfloat16)
            if turned < TURN - 1:
                cos, sin = rotated(cos, sin, turn[0, rows, :], turn[1, rows, :])
    for turned in range(TURN):
        source = slice(turned * part, (turned + 1) * part)
        for side, ref in enumerate((keep, other)):
            value = ref[source, :]
            swapped = pltpu.roll(value.astype(jnp.float32), LANES // 2, 1)
            data[turned, side * part : (side + 1) * part, :] = value
            data[turned, (2 + side) * part : (3 + side) * part, :] = jnp.where(
                right, -swapped, swapped
            ).astype(jnp.bfloat16)
    for turned in range(TURN):
        groups[turned] = jnp.dot(base[turned], data[turned], preferred_element_type=jnp.float32)

    def quarter(value):
        swapped = pltpu.roll(value, LANES // 2, 1)
        return jnp.where(right, -swapped, swapped)

    def fourths(values):
        low, high = values[0] + values[2], values[0] - values[2]
        odd, turned = values[1] + values[3], quarter(values[1] - values[3])
        return low + odd, high + turned, low - odd, high - turned

    zero = jnp.zeros((EDGE, LANES), jnp.float32)
    sub[:EDGE, :] = zero
    sub[EDGE + TURN * C :, :] = zero
    size = math.sqrt(0.5)
    for block in range(C // HALF):
        rows = slice(block * HALF, (block + 1) * HALF)
        evens = fourths([groups[turned, rows, :] for turned in range(0, TURN, 2)])
        odds = fourths([groups[turned, rows, :] for turned in range(1, TURN, 2)])
        second, fourth = quarter(odds[1]), quarter(odds[3])
        twisted = (
            odds[0],
            (odds[1] + second) * size,
            quarter(odds[2]),
            (fourth - odds[3]) * size,
        )
        for column in range(TURN // 2):
            for sign in range(2):
                value = evens[column] - twisted[column] if sign else evens[column] + twisted[column]
                begin = EDGE + (column + sign * TURN // 2) * C + block * HALF
                sub[begin : begin + HALF, :] = value


def pack_kernel(rep_count, places, sub, out):
    col_blocks = (C + 2 * EDGE) // PATCH
    lane = lanes_of((PATCH, LANES))
    fixed = lane - (lane // HALF) % SLOTS * HALF

    def pack(column, carry):
        begin = pl.multiple_of(column * C, C)
        blocks = [sub[pl.ds(begin + block * PATCH, PATCH), :] for block in range(col_blocks)]
        for rep in range(rep_count):
            mark = jnp.broadcast_to(places[column * rep_count + rep], (PATCH, LANES))
            source, wanted = fixed + (mark >> 3) * HALF, mark & 7
            total = jnp.zeros((PATCH, LANES), jnp.float32)
            for block in range(col_blocks):
                moved = jnp.take_along_axis(blocks[block], source, axis=1)
                total = jnp.where(wanted == block, moved, total)
            out[column * rep_count + rep] = total.astype(jnp.bfloat16)
        return carry

    lax.fori_loop(0, out.shape[0] // rep_count, pack, 0, unroll=True)


def taps_kernel(taps, vis_u, vis_v, taps_u, taps_v):
    length = vis_u.shape[-1]
    taps_u[...] = jnp.zeros_like(taps_u)

    def taps_of(offsets):
        distance = sublanes_of((PATCH, length)) - offsets
        value = jnp.zeros((PATCH, length), jnp.float32)
        for position in range(KW):
            value = jnp.where(distance == position, taps[position], value)
        return value

    for p in range(SLOTS):
        span = slice(p * length, (p + 1) * length)
        rows_u = taps_of(vis_u[0, p : p + 1, :])
        high = rows_u.astype(jnp.bfloat16)
        low = (rows_u - high.astype(jnp.float32)).astype(jnp.bfloat16)
        for half in range(2):
            begin = half * (LANES // 2) + p * HALF
            taps_u[begin : begin + HALF, span] = high[half * HALF : (half + 1) * HALF]
            taps_u[LANES + begin : LANES + begin + HALF, span] = low[
                half * HALF : (half + 1) * HALF
            ]
        taps_v[:, span] = taps_of(vis_v[0, p : p + 1, :])


def degrid_kernel(counts, place, arrived, observed, taps_u, taps_v, residual, out, weighted):
    length = observed.shape[-1]
    left = lanes_of((PATCH, LANES)) < LANES // 2
    sums = []
    for half in range(2):
        total = arrived[half].astype(jnp.float32)
        for source in range(half + 2, arrived.shape[0], 2):
            total = total + arrived[source].astype(jnp.float32)
        sums.append(total)
    swapped = [pltpu.roll(total, LANES // 2, 1) for total in sums]
    patch = jnp.concatenate(
        [jnp.where(left, sums[0], swapped[1]), jnp.where(left, swapped[0], sums[1])], axis=0
    ).astype(jnp.bfloat16)
    patch = jnp.concatenate([patch, patch], axis=1)
    for p in range(SLOTS):
        span = slice(p * length, (p + 1) * length)
        inner = jnp.dot(patch, taps_u[:, span], preferred_element_type=jnp.float32)
        rows_v = taps_v[:, span]
        live = lanes_of((1, length)) < counts[0:1, p : p + 1]
        for c in range(2):
            predicted = jnp.sum(inner[c * PATCH : (c + 1) * PATCH] * rows_v, axis=0, keepdims=True)
            value = jnp.where(live, observed[c, 0, p : p + 1, :] - predicted, 0.0)
            residual[c, 0, p : p + 1, :] = value
            value = value * rows_v
            high = value.astype(jnp.bfloat16)
            weighted[c * PATCH : (c + 1) * PATCH, span] = high
            weighted[2 * PATCH + c * PATCH : 2 * PATCH + (c + 1) * PATCH, span] = (
                value - high.astype(jnp.float32)
            ).astype(jnp.bfloat16)
    product = contract(weighted[...], taps_u[...])
    product = product[: 2 * PATCH] + product[2 * PATCH :]
    gridded = product[:, :LANES] + product[:, LANES:]
    parts = [gridded[:PATCH], gridded[PATCH:]]
    swapped = [pltpu.roll(part, LANES // 2, 1) for part in parts]
    halves = [jnp.where(left, parts[0], swapped[1]), jnp.where(left, swapped[0], parts[1])]
    row = place[...] >> 3
    owners = C // HALF
    for owner in range(owners):
        piece = jnp.where(row == owner // 2, halves[owner % 2], 0.0).astype(jnp.bfloat16)
        for first in range(0, out.shape[0], owners):
            out[first + owner] = piece


def return_kernel(
    rep_count, places, arrived, residual_near, residual, returned, canvas, sem
):
    copy = pltpu.make_async_copy(residual_near, residual, sem)
    copy.start()
    sub_cols = returned.shape[1]
    col_blocks = (C + 2 * EDGE) // PATCH
    for column in range(sub_cols):
        values, marks = [], []
        for rep in range(rep_count):
            device = column * rep_count + rep
            values.append(arrived[device].astype(jnp.float32))
            marks.append(places[device] & 7)
        for block in range(col_blocks):
            total = jnp.where(marks[0] == block, values[0], 0.0)
            for value, mark in zip(values[1:], marks[1:]):
                total = total + jnp.where(mark == block, value, 0.0)
            canvas[column * col_blocks + block] = total
    shape = (2 * HALF, LANES)
    row, lane = sublanes_of(shape), lanes_of(shape)
    picked = (row // HALF == lane // (LANES // 2)) & (row % HALF == lane % HALF)
    pick = jnp.where(picked, 1.0, 0.0).astype(jnp.bfloat16)
    pick = jnp.concatenate([pick, pick], axis=1)
    for column in range(sub_cols):
        blocks = [canvas[column * col_blocks + 1 + block] for block in range(C // PATCH)]
        if column > 0:
            blocks[0] = blocks[0] + canvas[column * col_blocks - 1]
        if column < sub_cols - 1:
            blocks[-1] = blocks[-1] + canvas[(column + 1) * col_blocks]
        total = jnp.concatenate(blocks, axis=0)
        high = total.astype(jnp.bfloat16)
        low = (total - high.astype(jnp.float32)).astype(jnp.bfloat16)
        value = contract(pick, jnp.concatenate([high, low], axis=1)).astype(jnp.bfloat16)
        for c in range(2):
            returned[c, column] = value[c * HALF : (c + 1) * HALF]
    copy.wait()


def call(kernel, out_shape, operands, scratch, flops, scalars=0, first=None, outs=None, limit=24):
    spaces = [pltpu.SMEM] * scalars + [pltpu.VMEM] * (len(operands) - scalars)
    if first is not None:
        spaces[0] = first
    single = not isinstance(out_shape, tuple)
    outs = outs or (pltpu.VMEM,) * (1 if single else len(out_shape))
    specs = tuple(pl.BlockSpec(memory_space=space) for space in outs)
    return pl.pallas_call(
        kernel,
        out_shape=out_shape,
        in_specs=[pl.BlockSpec(memory_space=space) for space in spaces],
        out_specs=specs[0] if single else specs,
        scratch_shapes=scratch,
        compiler_params=pltpu.CompilerParams(vmem_limit_bytes=limit << 20),
        cost_estimate=pl.CostEstimate(flops=flops, bytes_accessed=1 << 20, transcendentals=0),
    )(*operands)


def exchanged(value):
    return lax.all_to_all(value, EVERYONE, split_axis=0, concat_axis=0, tiled=True)


def fused(facets, taper, kernel, observed, patch_pos, counts, vis_u, vis_v):
    rep_count = lax.axis_size("rep")
    sub_cols = lax.axis_size("role") * lax.axis_size("grp")
    devices = sub_cols * rep_count
    count = facets.shape[2]
    length = observed.shape[-1]
    chunks = 4
    col_blocks = (C + 2 * EDGE) // PATCH
    f32, bf16 = jnp.float32, jnp.bfloat16

    place, copies = call(
        place_kernel,
        (pltpu.VMEM((1, LANES), jnp.int32), pltpu.VMEM((devices, 1, LANES), jnp.int32)),
        (patch_pos,),
        [],
        1 << 33,
    )
    places = exchanged(copies)
    places = near(places)
    strip = pltpu.VMEM((count, LANES), bf16)
    keep, send = call(
        lambda *refs: row_kernel(rep_count, *refs),
        (strip, strip),
        (far(facets), near(taper)) + tuple(near(jnp.asarray(table)) for table in row_tables()),
        [
            pltpu.VMEM((chunks, 2, count, F // chunks), bf16),
            pltpu.VMEM((chunks, 2 * C, F // chunks), bf16),
            pltpu.VMEM((chunks, 2 * C, F // chunks), bf16),
            pltpu.VMEM((2, C, LANES), f32),
            pltpu.VMEM((count, 2 * C), f32),
            pltpu.VMEM((8, LANES), f32),
            pltpu.VMEM((count, LANES), f32),
            pltpu.VMEM((count, LANES), f32),
            pltpu.SemaphoreType.DMA((chunks,)),
        ],
        8 * C * F * count,
        first=pltpu.HBM,
    )
    pairs = [(i, i + 1 - 2 * (i % 2)) for i in range(rep_count)]
    other = lax.ppermute(send, "rep", pairs)
    other = near(other)
    taps_u, taps_v = call(
        taps_kernel,
        (
            pltpu.VMEM((2 * LANES, SLOTS * length), bf16),
            pltpu.VMEM((PATCH, SLOTS * length), f32),
        ),
        (kernel, near(vis_u), near(vis_v)),
        [],
        1 << 26,
        scalars=1,
    )
    sub = call(
        lambda *refs: column_kernel(rep_count, *refs),
        pltpu.VMEM((sub_cols * C + 2 * EDGE, LANES), f32),
        (near(keep), other) + tuple(near(table) for table in column_tables()),
        [
            pltpu.VMEM((TURN, C, 2 * LANES), bf16),
            pltpu.VMEM((TURN, 2 * LANES, LANES), bf16),
            pltpu.VMEM((TURN, C, LANES), f32),
        ],
        1 << 20,
    )
    chunk = pltpu.VMEM((devices, PATCH, LANES), bf16)
    outgoing = call(
        lambda *refs: pack_kernel(rep_count, *refs), chunk, (places, near(sub)), [], 1 << 28
    )
    arrived = near(exchanged(outgoing))
    residual, gridded = call(
        degrid_kernel,
        (pltpu.VMEM(observed.shape, f32), chunk),
        (near(counts), place, arrived, near(observed), near(taps_u), near(taps_v)),
        [pltpu.VMEM((4 * PATCH, SLOTS * length), bf16)],
        1 << 28,
    )
    spread = near(exchanged(gridded))
    return call(
        lambda *refs: return_kernel(rep_count, *refs),
        (
            pltpu.HBM(observed.shape, f32),
            jax.ShapeDtypeStruct((2, sub_cols, HALF, C), bf16),
        ),
        (places, spread, near(residual)),
        [
            pltpu.VMEM((sub_cols * col_blocks, PATCH, LANES), f32),
            pltpu.SemaphoreType.DMA,
        ],
        1 << 26,
        outs=(pltpu.HBM, pltpu.VMEM),
    )


def part(facets, taper, kernel, observed, patch_pos, counts, vis_u, vis_v):
    grp_count = lax.axis_size("grp")
    rep_count = lax.axis_size("rep")
    owners = grp_count * rep_count
    sub_cols = lax.axis_size("role") * grp_count
    whole = (
        owners * HALF == C
        and owners == TURN
        and sub_cols == TURN
        and facets.shape[2] * TURN == F
        and rep_count % 2 == 0
        and patch_pos.shape[1] == SLOTS
        and facets.shape[2] == TURN * LANES // 2
        and observed.shape[-1] % LANES == 0
    )
    path = fused if whole else local
    return path(facets, taper, kernel, observed, patch_pos, counts, vis_u, vis_v)


def solution(mesh):
    return jax.shard_map(
        part,
        mesh=mesh,
        in_specs=(
            P("role", None, ("grp", "rep"), None),
            P("role", None),
            P(),
            P(None, ("role", "grp"), "rep", None),
            P(("role", "grp"), "rep"),
            P(("role", "grp"), "rep"),
            P(("role", "grp"), "rep", None),
            P(("role", "grp"), "rep", None),
        ),
        out_specs=(P(None, ("role", "grp"), "rep", None), P(None, None, ("grp", "rep"), None)),
        check_vma=False,
    )
```

```python
import math

import jax
import numpy as np
import jax.numpy as jnp
from jax import lax
from jax.experimental import pallas as pl
from jax.experimental.pallas import tpu as pltpu
from jax.sharding import PartitionSpec as P


F = 4096
C = 128
PATCH = 32
EDGE = 32
KW = 8


def extended(block, sides, width):
    for axis, dim in sides:
        count = lax.axis_size(axis)
        forward = [(i, i + 1) for i in range(count - 1)]
        backward = [(target, source) for source, target in forward]
        low = lax.ppermute(
            lax.slice_in_dim(block, block.shape[dim] - width, None, axis=dim), axis, forward
        )
        high = lax.ppermute(lax.slice_in_dim(block, 0, width, axis=dim), axis, backward)
        block = jnp.concatenate([low, block, high], axis=dim)
    return block


def shifted(value, axis, by):
    size = lax.axis_size(axis)
    pairs = [(i, i + by) for i in range(size) if 0 <= i + by < size]
    return lax.ppermute(value, axis, pairs)


def phases(frequency, length):
    columns = jnp.arange(length, dtype=jnp.int32)
    product = frequency[:, None] * columns[None, :] % length
    angles = product.astype(jnp.float32) * (2.0 * math.pi / length)
    return (jnp.cos(angles), jnp.sin(angles))


def windowed(frequency, window):
    length = window.shape[0]
    wave_cos, wave_sin = phases(frequency, length)
    scale_norm = 1.0 / math.sqrt(length)
    table_re = (window[None, :] * wave_cos * scale_norm).astype(jnp.bfloat16)
    table_im = (-(window[None, :] * wave_sin) * scale_norm).astype(jnp.bfloat16)
    return (table_re, table_im)


def contract(left, right):
    return lax.dot_general(
        left, right, (((1,), (1,)), ((), ())), preferred_element_type=jnp.float32
    )


def project(table_re, table_im, data_re, data_im):
    part_re = contract(table_re, data_re) - contract(table_im, data_im)
    part_im = contract(table_re, data_im) + contract(table_im, data_re)
    return (part_re, part_im)


def modulate(part_re, part_im, wave_cos, wave_sin):
    mod_re = (part_re * wave_cos + part_im * wave_sin).astype(jnp.bfloat16)
    mod_im = (part_im * wave_cos - part_re * wave_sin).astype(jnp.bfloat16)
    return (mod_re, mod_im)


def kernel_rows(offsets, kernel):
    cell_index = jnp.arange(PATCH, dtype=jnp.int32)
    distance = cell_index[None, :, None] - offsets[:, None, :]
    result = jnp.zeros(distance.shape, jnp.float32)
    for position in range(KW):
        result = result + kernel[position] * (distance == position).astype(jnp.float32)
    return result


def degrid(widened, patch_pos, counts, vis_u, vis_v, observed, kernel):
    high = lax.Precision.HIGHEST
    row_blocks = widened.shape[1] // PATCH
    col_blocks = widened.shape[2] // PATCH
    blocks = widened.reshape(2, row_blocks, PATCH, col_blocks, PATCH).transpose(0, 1, 3, 2, 4)
    blocks = blocks.reshape(2, row_blocks * col_blocks, PATCH, PATCH)
    selected = jnp.take(blocks, patch_pos, axis=1).astype(jnp.float32)
    rows_u = kernel_rows(vis_u, kernel)
    rows_v = kernel_rows(vis_v, kernel)
    partial_value = jnp.einsum("cpab,pav->cpbv", selected, rows_u, precision=high)
    predicted = jnp.einsum("cpbv,pbv->cpv", partial_value, rows_v, precision=high)
    live_mask = (jnp.arange(observed.shape[-1], dtype=jnp.int32)[None, :] < counts[:, None]).astype(
        jnp.float32
    )
    residual = (observed - predicted) * live_mask[None]
    weighted = residual[:, :, None, :] * rows_v[None]
    gridded = jnp.einsum("pav,cpbv->cpab", rows_u, weighted, precision=high)
    one_hot = (
        patch_pos[:, None] == jnp.arange(row_blocks * col_blocks, dtype=jnp.int32)[None, :]
    ).astype(jnp.float32)
    placed = jnp.einsum("pq,cpab->cqab", one_hot, gridded, precision=high)
    regrid = placed.reshape(2, row_blocks, col_blocks, PATCH, PATCH).transpose(0, 1, 3, 2, 4)
    return (residual, regrid.reshape(2, widened.shape[1], widened.shape[2]))


def local(facets, taper, kernel, observed, patch_pos, counts, vis_u, vis_v):
    grp_count = lax.axis_size("grp")
    rep_count = lax.axis_size("rep")
    role_count = lax.axis_size("role")
    sub_cols = role_count * grp_count
    row_share = C // (grp_count * rep_count)
    strip_data = facets[0]
    window = taper[0]
    row_freq = jnp.arange(C, dtype=jnp.int32)
    table_re, table_im = windowed(row_freq, window)
    part_re, part_im = project(table_re, table_im, strip_data[0], strip_data[1])
    partial_value = jnp.stack([part_re, part_im]).astype(jnp.bfloat16)
    row_block = lax.all_to_all(
        partial_value, ("grp", "rep"), split_axis=1, concat_axis=2, tiled=True
    )
    shift_freq = jnp.arange(sub_cols, dtype=jnp.int32) * (F // sub_cols)
    wave_cos, wave_sin = phases(shift_freq, F)
    mod_re, mod_im = modulate(
        row_block[0][None].astype(jnp.float32),
        row_block[1][None].astype(jnp.float32),
        (window[None, :] * wave_cos)[:, None, :],
        (window[None, :] * wave_sin)[:, None, :],
    )
    base_re, base_im = windowed(jnp.arange(C, dtype=jnp.int32), jnp.ones((F,), jnp.float32))
    q_re, q_im = project(
        mod_re.reshape(sub_cols * row_share, F),
        mod_im.reshape(sub_cols * row_share, F),
        base_re,
        base_im,
    )
    contrib = jnp.stack([q_re, q_im]).astype(jnp.bfloat16).reshape(2, sub_cols, row_share, C)
    arrived = lax.all_to_all(contrib, ("role", "grp"), split_axis=1, concat_axis=2, tiled=True)
    arrived = arrived.reshape(2, role_count, grp_count, row_share, C).astype(jnp.float32)
    quarter = jnp.sum(arrived, axis=1).astype(jnp.bfloat16)
    collected_rows = lax.all_gather(quarter[:, :, None], "rep", axis=2, tiled=True)
    subgrid = collected_rows.reshape(2, C, C)
    widened = extended(subgrid, ((("role", "grp"), 2),), EDGE)
    residual, regrid = degrid(
        widened, patch_pos[0], counts[0], vis_u[0], vis_v[0], observed[:, 0], kernel
    )
    left_part = regrid[:, :, :EDGE]
    right_part = regrid[:, :, EDGE + C :]
    center = regrid[:, :, EDGE : EDGE + C]
    from_right = shifted(left_part.astype(jnp.bfloat16), ("role", "grp"), -1).astype(
        left_part.dtype
    )
    from_left = shifted(right_part.astype(jnp.bfloat16), ("role", "grp"), 1).astype(
        right_part.dtype
    )
    resid = center.at[:, :, :EDGE].add(from_left).at[:, :, C - EDGE :].add(from_right)
    pieces = resid.reshape(2, grp_count * rep_count, row_share, C)
    spread = lax.all_to_all(
        pieces.astype(jnp.bfloat16), ("grp", "rep"), split_axis=1, concat_axis=1, tiled=True
    ).astype(pieces.dtype)
    owned = jnp.sum(spread.reshape(2, grp_count, rep_count, row_share, C), axis=2).astype(
        jnp.bfloat16
    )
    returned = lax.all_gather(owned, "role", axis=1, tiled=True)
    return (residual[:, None], returned)


LANES = 128
HALF = PATCH // 2
SLOTS = LANES // (2 * HALF)
TURN = 8
EVERYONE = ("role", "grp", "rep")


def lanes_of(shape):
    return lax.broadcasted_iota(jnp.int32, shape, len(shape) - 1)


def sublanes_of(shape):
    return lax.broadcasted_iota(jnp.int32, shape, len(shape) - 2)


def near(value):
    return pltpu.with_memory_space_constraint(value, pltpu.VMEM)


def far(value):
    return pltpu.with_memory_space_constraint(value, pltpu.HBM)


def waves(cells, scale):
    angles = np.arange(C)[:, None] * cells[None, :] % F * (2.0 * np.pi / F)
    return np.stack([np.cos(angles) * scale, np.sin(angles) * scale]).astype(np.float32)


def row_tables():
    cells = np.arange(LANES)
    return waves(cells, 1.0 / math.sqrt(F)), waves(np.full(LANES, LANES), 1.0)


def column_tables():
    cells = np.arange(LANES) % (LANES // 2) * TURN
    return waves(cells, 1.0 / math.sqrt(F)), waves(np.ones(LANES, np.int64), 1.0)


def eighth(index):
    def cosine(turn):
        turn = turn & 7
        size = jnp.where((turn & 1) == 1, math.sqrt(0.5), jnp.where((turn & 3) == 0, 1.0, 0.0))
        return jnp.where((turn > 2) & (turn < 6), -size, size).astype(jnp.float32)

    return cosine(index), cosine(index + 6)


def rotated(cos, sin, turn_cos, turn_sin):
    return cos * turn_cos - sin * turn_sin, sin * turn_cos + cos * turn_sin


def place_kernel(positions, place, copies):
    col_blocks = (C + 2 * EDGE) // PATCH
    slot = (lanes_of((1, LANES)) // HALF) % SLOTS
    value = jnp.zeros((1, LANES), jnp.int32)
    for p in range(SLOTS):
        value = jnp.where(slot == p, positions[0:1, p : p + 1], value)
    row = sum(jnp.where(value >= block * col_blocks, 1, 0) for block in range(1, C // PATCH))
    value = row * (8 - col_blocks) + value
    place[...] = value
    copies[...] = jnp.broadcast_to(value[None], copies.shape)


def row_kernel(
    rep_count, facets, taper, start, turn, keep, send, data, table_a, table_b,
    wave, total, strip, first_rows, second_rows, sems,
):
    chunks, _, width = table_a.shape
    count = keep.shape[0]

    def fetch(chunk):
        columns = pl.ds(pl.multiple_of(chunk * width, width), width)
        return pltpu.make_async_copy(
            facets.at[0, :, :, columns], data.at[chunk], sems.at[chunk]
        )

    fetch(0).start()
    fetch(1).start()
    wave[...] = start[...]
    total[...] = jnp.zeros_like(total)

    def build(step, carry):
        chunk, piece = step // (width // LANES), step % (width // LANES)
        window = taper[:, pl.ds(pl.multiple_of(step * LANES, LANES), LANES)]
        columns = pl.ds(pl.multiple_of(piece * LANES, LANES), LANES)
        for block in range(C // HALF):
            rows = slice(block * HALF, (block + 1) * HALF)
            cos, sin = wave[0, rows, :], wave[1, rows, :]
            re = window * cos
            im = window * sin
            base = (block % 2) * C + (block // 2) * HALF
            low = slice(base, base + HALF)
            high = slice(base + C // 2, base + C // 2 + HALF)
            table_a[chunk, low, columns] = re.astype(jnp.bfloat16)
            table_a[chunk, high, columns] = (-im).astype(jnp.bfloat16)
            table_b[chunk, low, columns] = im.astype(jnp.bfloat16)
            table_b[chunk, high, columns] = re.astype(jnp.bfloat16)
            cos, sin = rotated(cos, sin, turn[0, rows, :], turn[1, rows, :])
            wave[0, rows, :] = cos
            wave[1, rows, :] = sin
        return carry

    lax.fori_loop(0, chunks * (width // LANES), build, 0)

    def multiply(chunk, carry):
        fetch(chunk).wait()

        @pl.when(chunk + 2 < chunks)
        def _():
            fetch(chunk + 2).start()

        total[...] += contract(data[chunk, 0], table_a[chunk]) + contract(
            data[chunk, 1], table_b[chunk]
        )
        return carry

    lax.fori_loop(0, chunks, multiply, 0)
    place = lax.axis_index("grp") * rep_count + lax.axis_index("rep")
    for piece in range(count // LANES):
        offset = pl.multiple_of(place * count + piece * LANES, LANES)
        strip[piece : piece + 1, :] = taper[:, pl.ds(offset, LANES)]
    window = jnp.transpose(strip[...])
    for piece in range(count // LANES):
        rows = slice(piece * LANES, (piece + 1) * LANES)
        scaled = total[rows, :] * window[:, piece : piece + 1]
        first_rows[rows, :] = scaled[:, :C]
        second_rows[rows, :] = scaled[:, C:]
    even = lax.rem(lax.axis_index("rep"), 2) == 0
    part = count // TURN
    for turned in range(TURN):
        rows = pl.ds(turned, part, stride=TURN)
        first, second = first_rows[rows, :], second_rows[rows, :]
        target = slice(turned * part, (turned + 1) * part)
        keep[target, :] = jnp.where(even, first, second).astype(jnp.bfloat16)
        send[target, :] = jnp.where(even, second, first).astype(jnp.bfloat16)


def column_kernel(rep_count, keep, other, start, turn, sub, base, data, groups):
    part = keep.shape[0] // TURN
    mine = lax.axis_index("grp") * rep_count + lax.axis_index("rep")
    near_by = mine + 1 - 2 * lax.rem(mine, 2)
    shape = (HALF, LANES)
    right = lanes_of((1, LANES)) >= LANES // 2
    place = jnp.where(lanes_of(shape) < LANES // 2, mine, near_by)
    phase_cos, phase_sin = eighth((sublanes_of(shape) & 7) * place)
    for block in range(C // HALF):
        rows = slice(block * HALF, (block + 1) * HALF)
        cos, sin = rotated(start[0, rows, :], start[1, rows, :], phase_cos, phase_sin)
        for turned in range(TURN):
            base[turned, rows, :LANES] = cos.astype(jnp.bfloat16)
            base[turned, rows, LANES:] = sin.astype(jnp.bfloat16)
            if turned < TURN - 1:
                cos, sin = rotated(cos, sin, turn[0, rows, :], turn[1, rows, :])
    for turned in range(TURN):
        source = slice(turned * part, (turned + 1) * part)
        for side, ref in enumerate((keep, other)):
            value = ref[source, :]
            swapped = pltpu.roll(value.astype(jnp.float32), LANES // 2, 1)
            data[turned, side * part : (side + 1) * part, :] = value
            data[turned, (2 + side) * part : (3 + side) * part, :] = jnp.where(
                right, -swapped, swapped
            ).astype(jnp.bfloat16)
    for turned in range(TURN):
        groups[turned] = jnp.dot(base[turned], data[turned], preferred_element_type=jnp.float32)

    def quarter(value):
        swapped = pltpu.roll(value, LANES // 2, 1)
        return jnp.where(right, -swapped, swapped)

    def fourths(values):
        low, high = values[0] + values[2], values[0] - values[2]
        odd, turned = values[1] + values[3], quarter(values[1] - values[3])
        return low + odd, high + turned, low - odd, high - turned

    zero = jnp.zeros((EDGE, LANES), jnp.float32)
    sub[:EDGE, :] = zero
    sub[EDGE + TURN * C :, :] = zero
    size = math.sqrt(0.5)
    for block in range(C // HALF):
        rows = slice(block * HALF, (block + 1) * HALF)
        evens = fourths([groups[turned, rows, :] for turned in range(0, TURN, 2)])
        odds = fourths([groups[turned, rows, :] for turned in range(1, TURN, 2)])
        second, fourth = quarter(odds[1]), quarter(odds[3])
        twisted = (
            odds[0],
            (odds[1] + second) * size,
            quarter(odds[2]),
            (fourth - odds[3]) * size,
        )
        for column in range(TURN // 2):
            for sign in range(2):
                value = evens[column] - twisted[column] if sign else evens[column] + twisted[column]
                begin = EDGE + (column + sign * TURN // 2) * C + block * HALF
                sub[begin : begin + HALF, :] = value


def pack_kernel(rep_count, places, sub, out):
    col_blocks = (C + 2 * EDGE) // PATCH
    lane = lanes_of((PATCH, LANES))
    fixed = lane - (lane // HALF) % SLOTS * HALF

    def pack(column, carry):
        begin = pl.multiple_of(column * C, C)
        blocks = [sub[pl.ds(begin + block * PATCH, PATCH), :] for block in range(col_blocks)]
        for rep in range(rep_count):
            mark = jnp.broadcast_to(places[column * rep_count + rep], (PATCH, LANES))
            source, wanted = fixed + (mark >> 3) * HALF, mark & 7
            total = jnp.zeros((PATCH, LANES), jnp.float32)
            for block in range(col_blocks):
                moved = jnp.take_along_axis(blocks[block], source, axis=1)
                total = jnp.where(wanted == block, moved, total)
            out[column * rep_count + rep] = total.astype(jnp.bfloat16)
        return carry

    lax.fori_loop(0, out.shape[0] // rep_count, pack, 0, unroll=True)


def taps_kernel(taps, vis_u, vis_v, taps_u, taps_v):
    length = vis_u.shape[-1]
    taps_u[...] = jnp.zeros_like(taps_u)

    def taps_of(offsets):
        distance = sublanes_of((PATCH, length)) - offsets
        value = jnp.zeros((PATCH, length), jnp.float32)
        for position in range(KW):
            value = jnp.where(distance == position, taps[position], value)
        return value

    for p in range(SLOTS):
        span = slice(p * length, (p + 1) * length)
        rows_u = taps_of(vis_u[0, p : p + 1, :])
        high = rows_u.astype(jnp.bfloat16)
        low = (rows_u - high.astype(jnp.float32)).astype(jnp.bfloat16)
        for half in range(2):
            begin = half * (LANES // 2) + p * HALF
            taps_u[begin : begin + HALF, span] = high[half * HALF : (half + 1) * HALF]
            taps_u[LANES + begin : LANES + begin + HALF, span] = low[
                half * HALF : (half + 1) * HALF
            ]
        taps_v[:, span] = taps_of(vis_v[0, p : p + 1, :])


def degrid_kernel(counts, place, arrived, observed, taps_u, taps_v, residual, out, weighted):
    length = observed.shape[-1]
    left = lanes_of((PATCH, LANES)) < LANES // 2
    sums = []
    for half in range(2):
        total = arrived[half].astype(jnp.float32)
        for source in range(half + 2, arrived.shape[0], 2):
            total = total + arrived[source].astype(jnp.float32)
        sums.append(total)
    swapped = [pltpu.roll(total, LANES // 2, 1) for total in sums]
    patch = jnp.concatenate(
        [jnp.where(left, sums[0], swapped[1]), jnp.where(left, swapped[0], sums[1])], axis=0
    ).astype(jnp.bfloat16)
    patch = jnp.concatenate([patch, patch], axis=1)
    for p in range(SLOTS):
        span = slice(p * length, (p + 1) * length)
        inner = jnp.dot(patch, taps_u[:, span], preferred_element_type=jnp.float32)
        rows_v = taps_v[:, span]
        live = lanes_of((1, length)) < counts[0:1, p : p + 1]
        for c in range(2):
            predicted = jnp.sum(inner[c * PATCH : (c + 1) * PATCH] * rows_v, axis=0, keepdims=True)
            value = jnp.where(live, observed[c, 0, p : p + 1, :] - predicted, 0.0)
            residual[c, 0, p : p + 1, :] = value
            value = value * rows_v
            high = value.astype(jnp.bfloat16)
            weighted[c * PATCH : (c + 1) * PATCH, span] = high
            weighted[2 * PATCH + c * PATCH : 2 * PATCH + (c + 1) * PATCH, span] = (
                value - high.astype(jnp.float32)
            ).astype(jnp.bfloat16)
    product = contract(weighted[...], taps_u[...])
    product = product[: 2 * PATCH] + product[2 * PATCH :]
    gridded = product[:, :LANES] + product[:, LANES:]
    parts = [gridded[:PATCH], gridded[PATCH:]]
    swapped = [pltpu.roll(part, LANES // 2, 1) for part in parts]
    halves = [jnp.where(left, parts[0], swapped[1]), jnp.where(left, swapped[0], parts[1])]
    row = place[...] >> 3
    owners = C // HALF
    for owner in range(owners):
        piece = jnp.where(row == owner // 2, halves[owner % 2], 0.0).astype(jnp.bfloat16)
        for first in range(0, out.shape[0], owners):
            out[first + owner] = piece


def return_kernel(
    rep_count, places, arrived, residual_near, residual, returned_far, canvas, returned, sem, sems
):
    copies = [pltpu.make_async_copy(residual_near, residual, sem)]
    copies[0].start()
    sub_cols = returned.shape[1]
    col_blocks = (C + 2 * EDGE) // PATCH
    for column in range(sub_cols):
        values, marks = [], []
        for rep in range(rep_count):
            device = column * rep_count + rep
            values.append(arrived[device].astype(jnp.float32))
            marks.append(places[device] & 7)
        for block in range(col_blocks):
            total = jnp.where(marks[0] == block, values[0], 0.0)
            for value, mark in zip(values[1:], marks[1:]):
                total = total + jnp.where(mark == block, value, 0.0)
            canvas[column * col_blocks + block] = total
    shape = (2 * HALF, LANES)
    row, lane = sublanes_of(shape), lanes_of(shape)
    picked = (row // HALF == lane // (LANES // 2)) & (row % HALF == lane % HALF)
    pick = jnp.where(picked, 1.0, 0.0).astype(jnp.bfloat16)
    pick = jnp.concatenate([pick, pick], axis=1)
    for column in range(sub_cols):
        blocks = [canvas[column * col_blocks + 1 + block] for block in range(C // PATCH)]
        if column > 0:
            blocks[0] = blocks[0] + canvas[column * col_blocks - 1]
        if column < sub_cols - 1:
            blocks[-1] = blocks[-1] + canvas[(column + 1) * col_blocks]
        total = jnp.concatenate(blocks, axis=0)
        high = total.astype(jnp.bfloat16)
        low = (total - high.astype(jnp.float32)).astype(jnp.bfloat16)
        value = contract(pick, jnp.concatenate([high, low], axis=1)).astype(jnp.bfloat16)
        for c in range(2):
            returned[c, column] = value[c * HALF : (c + 1) * HALF]
        if column % 4 == 3:
            columns = slice(column - 3, column + 1)
            copies.append(
                pltpu.make_async_copy(
                    returned.at[:, columns], returned_far.at[:, columns], sems.at[column // 4]
                )
            )
            copies[-1].start()
    for copy in copies:
        copy.wait()


def call(kernel, out_shape, operands, scratch, flops, scalars=0, first=None, outs=None, limit=24):
    spaces = [pltpu.SMEM] * scalars + [pltpu.VMEM] * (len(operands) - scalars)
    if first is not None:
        spaces[0] = first
    single = not isinstance(out_shape, tuple)
    outs = outs or (pltpu.VMEM,) * (1 if single else len(out_shape))
    specs = tuple(pl.BlockSpec(memory_space=space) for space in outs)
    return pl.pallas_call(
        kernel,
        out_shape=out_shape,
        in_specs=[pl.BlockSpec(memory_space=space) for space in spaces],
        out_specs=specs[0] if single else specs,
        scratch_shapes=scratch,
        compiler_params=pltpu.CompilerParams(vmem_limit_bytes=limit << 20),
        cost_estimate=pl.CostEstimate(flops=flops, bytes_accessed=1 << 20, transcendentals=0),
    )(*operands)


def exchanged(value):
    return lax.all_to_all(value, EVERYONE, split_axis=0, concat_axis=0, tiled=True)


def fused(facets, taper, kernel, observed, patch_pos, counts, vis_u, vis_v):
    rep_count = lax.axis_size("rep")
    sub_cols = lax.axis_size("role") * lax.axis_size("grp")
    devices = sub_cols * rep_count
    count = facets.shape[2]
    length = observed.shape[-1]
    chunks = 4
    col_blocks = (C + 2 * EDGE) // PATCH
    f32, bf16 = jnp.float32, jnp.bfloat16

    place, copies = call(
        place_kernel,
        (pltpu.VMEM((1, LANES), jnp.int32), pltpu.VMEM((devices, 1, LANES), jnp.int32)),
        (patch_pos,),
        [],
        1 << 33,
    )
    places = exchanged(copies)
    places = near(places)
    strip = pltpu.VMEM((count, LANES), bf16)
    keep, send = call(
        lambda *refs: row_kernel(rep_count, *refs),
        (strip, strip),
        (far(facets), near(taper)) + tuple(near(jnp.asarray(table)) for table in row_tables()),
        [
            pltpu.VMEM((chunks, 2, count, F // chunks), bf16),
            pltpu.VMEM((chunks, 2 * C, F // chunks), bf16),
            pltpu.VMEM((chunks, 2 * C, F // chunks), bf16),
            pltpu.VMEM((2, C, LANES), f32),
            pltpu.VMEM((count, 2 * C), f32),
            pltpu.VMEM((8, LANES), f32),
            pltpu.VMEM((count, LANES), f32),
            pltpu.VMEM((count, LANES), f32),
            pltpu.SemaphoreType.DMA((chunks,)),
        ],
        8 * C * F * count,
        first=pltpu.HBM,
    )
    pairs = [(i, i + 1 - 2 * (i % 2)) for i in range(rep_count)]
    other = lax.ppermute(send, "rep", pairs)
    other = near(other)
    taps_u, taps_v = call(
        taps_kernel,
        (
            pltpu.VMEM((2 * LANES, SLOTS * length), bf16),
            pltpu.VMEM((PATCH, SLOTS * length), f32),
        ),
        (kernel, near(vis_u), near(vis_v)),
        [],
        1 << 26,
        scalars=1,
    )
    sub = call(
        lambda *refs: column_kernel(rep_count, *refs),
        pltpu.VMEM((sub_cols * C + 2 * EDGE, LANES), f32),
        (near(keep), other) + tuple(near(table) for table in column_tables()),
        [
            pltpu.VMEM((TURN, C, 2 * LANES), bf16),
            pltpu.VMEM((TURN, 2 * LANES, LANES), bf16),
            pltpu.VMEM((TURN, C, LANES), f32),
        ],
        1 << 20,
    )
    chunk = pltpu.VMEM((devices, PATCH, LANES), bf16)
    outgoing = call(
        lambda *refs: pack_kernel(rep_count, *refs), chunk, (places, near(sub)), [], 1 << 28
    )
    arrived = near(exchanged(outgoing))
    residual, gridded = call(
        degrid_kernel,
        (pltpu.VMEM(observed.shape, f32), chunk),
        (near(counts), place, arrived, near(observed), near(taps_u), near(taps_v)),
        [pltpu.VMEM((4 * PATCH, SLOTS * length), bf16)],
        1 << 28,
    )
    spread = near(exchanged(gridded))
    return call(
        lambda *refs: return_kernel(rep_count, *refs),
        (
            pltpu.HBM(observed.shape, f32),
            pltpu.HBM((2, sub_cols, HALF, C), bf16),
        ),
        (places, spread, near(residual)),
        [
            pltpu.VMEM((sub_cols * col_blocks, PATCH, LANES), f32),
            pltpu.VMEM((2, sub_cols, HALF, C), bf16),
            pltpu.SemaphoreType.DMA,
            pltpu.SemaphoreType.DMA((sub_cols // 4,)),
        ],
        1 << 26,
        outs=(pltpu.HBM, pltpu.HBM),
    )


def part(facets, taper, kernel, observed, patch_pos, counts, vis_u, vis_v):
    grp_count = lax.axis_size("grp")
    rep_count = lax.axis_size("rep")
    owners = grp_count * rep_count
    sub_cols = lax.axis_size("role") * grp_count
    whole = (
        owners * HALF == C
        and owners == TURN
        and sub_cols == TURN
        and facets.shape[2] * TURN == F
        and rep_count % 2 == 0
        and patch_pos.shape[1] == SLOTS
        and facets.shape[2] == TURN * LANES // 2
        and observed.shape[-1] % LANES == 0
    )
    path = fused if whole else local
    return path(facets, taper, kernel, observed, patch_pos, counts, vis_u, vis_v)


def solution(mesh):
    return jax.shard_map(
        part,
        mesh=mesh,
        in_specs=(
            P("role", None, ("grp", "rep"), None),
            P("role", None),
            P(),
            P(None, ("role", "grp"), "rep", None),
            P(("role", "grp"), "rep"),
            P(("role", "grp"), "rep"),
            P(("role", "grp"), "rep", None),
            P(("role", "grp"), "rep", None),
        ),
        out_specs=(P(None, ("role", "grp"), "rep", None), P(None, None, ("grp", "rep"), None)),
        check_vma=False,
    )
```

```python
import math

import jax
import numpy as np
import jax.numpy as jnp
from jax import lax
from jax.experimental import pallas as pl
from jax.experimental.pallas import tpu as pltpu
from jax.sharding import PartitionSpec as P


F = 4096
C = 128
PATCH = 32
EDGE = 32
KW = 8


def extended(block, sides, width):
    for axis, dim in sides:
        count = lax.axis_size(axis)
        forward = [(i, i + 1) for i in range(count - 1)]
        backward = [(target, source) for source, target in forward]
        low = lax.ppermute(
            lax.slice_in_dim(block, block.shape[dim] - width, None, axis=dim), axis, forward
        )
        high = lax.ppermute(lax.slice_in_dim(block, 0, width, axis=dim), axis, backward)
        block = jnp.concatenate([low, block, high], axis=dim)
    return block


def shifted(value, axis, by):
    size = lax.axis_size(axis)
    pairs = [(i, i + by) for i in range(size) if 0 <= i + by < size]
    return lax.ppermute(value, axis, pairs)


def phases(frequency, length):
    columns = jnp.arange(length, dtype=jnp.int32)
    product = frequency[:, None] * columns[None, :] % length
    angles = product.astype(jnp.float32) * (2.0 * math.pi / length)
    return (jnp.cos(angles), jnp.sin(angles))


def windowed(frequency, window):
    length = window.shape[0]
    wave_cos, wave_sin = phases(frequency, length)
    scale_norm = 1.0 / math.sqrt(length)
    table_re = (window[None, :] * wave_cos * scale_norm).astype(jnp.bfloat16)
    table_im = (-(window[None, :] * wave_sin) * scale_norm).astype(jnp.bfloat16)
    return (table_re, table_im)


def contract(left, right):
    return lax.dot_general(
        left, right, (((1,), (1,)), ((), ())), preferred_element_type=jnp.float32
    )


def project(table_re, table_im, data_re, data_im):
    part_re = contract(table_re, data_re) - contract(table_im, data_im)
    part_im = contract(table_re, data_im) + contract(table_im, data_re)
    return (part_re, part_im)


def modulate(part_re, part_im, wave_cos, wave_sin):
    mod_re = (part_re * wave_cos + part_im * wave_sin).astype(jnp.bfloat16)
    mod_im = (part_im * wave_cos - part_re * wave_sin).astype(jnp.bfloat16)
    return (mod_re, mod_im)


def kernel_rows(offsets, kernel):
    cell_index = jnp.arange(PATCH, dtype=jnp.int32)
    distance = cell_index[None, :, None] - offsets[:, None, :]
    result = jnp.zeros(distance.shape, jnp.float32)
    for position in range(KW):
        result = result + kernel[position] * (distance == position).astype(jnp.float32)
    return result


def degrid(widened, patch_pos, counts, vis_u, vis_v, observed, kernel):
    high = lax.Precision.HIGHEST
    row_blocks = widened.shape[1] // PATCH
    col_blocks = widened.shape[2] // PATCH
    blocks = widened.reshape(2, row_blocks, PATCH, col_blocks, PATCH).transpose(0, 1, 3, 2, 4)
    blocks = blocks.reshape(2, row_blocks * col_blocks, PATCH, PATCH)
    selected = jnp.take(blocks, patch_pos, axis=1).astype(jnp.float32)
    rows_u = kernel_rows(vis_u, kernel)
    rows_v = kernel_rows(vis_v, kernel)
    partial_value = jnp.einsum("cpab,pav->cpbv", selected, rows_u, precision=high)
    predicted = jnp.einsum("cpbv,pbv->cpv", partial_value, rows_v, precision=high)
    live_mask = (jnp.arange(observed.shape[-1], dtype=jnp.int32)[None, :] < counts[:, None]).astype(
        jnp.float32
    )
    residual = (observed - predicted) * live_mask[None]
    weighted = residual[:, :, None, :] * rows_v[None]
    gridded = jnp.einsum("pav,cpbv->cpab", rows_u, weighted, precision=high)
    one_hot = (
        patch_pos[:, None] == jnp.arange(row_blocks * col_blocks, dtype=jnp.int32)[None, :]
    ).astype(jnp.float32)
    placed = jnp.einsum("pq,cpab->cqab", one_hot, gridded, precision=high)
    regrid = placed.reshape(2, row_blocks, col_blocks, PATCH, PATCH).transpose(0, 1, 3, 2, 4)
    return (residual, regrid.reshape(2, widened.shape[1], widened.shape[2]))


def local(facets, taper, kernel, observed, patch_pos, counts, vis_u, vis_v):
    grp_count = lax.axis_size("grp")
    rep_count = lax.axis_size("rep")
    role_count = lax.axis_size("role")
    sub_cols = role_count * grp_count
    row_share = C // (grp_count * rep_count)
    strip_data = facets[0]
    window = taper[0]
    row_freq = jnp.arange(C, dtype=jnp.int32)
    table_re, table_im = windowed(row_freq, window)
    part_re, part_im = project(table_re, table_im, strip_data[0], strip_data[1])
    partial_value = jnp.stack([part_re, part_im]).astype(jnp.bfloat16)
    row_block = lax.all_to_all(
        partial_value, ("grp", "rep"), split_axis=1, concat_axis=2, tiled=True
    )
    shift_freq = jnp.arange(sub_cols, dtype=jnp.int32) * (F // sub_cols)
    wave_cos, wave_sin = phases(shift_freq, F)
    mod_re, mod_im = modulate(
        row_block[0][None].astype(jnp.float32),
        row_block[1][None].astype(jnp.float32),
        (window[None, :] * wave_cos)[:, None, :],
        (window[None, :] * wave_sin)[:, None, :],
    )
    base_re, base_im = windowed(jnp.arange(C, dtype=jnp.int32), jnp.ones((F,), jnp.float32))
    q_re, q_im = project(
        mod_re.reshape(sub_cols * row_share, F),
        mod_im.reshape(sub_cols * row_share, F),
        base_re,
        base_im,
    )
    contrib = jnp.stack([q_re, q_im]).astype(jnp.bfloat16).reshape(2, sub_cols, row_share, C)
    arrived = lax.all_to_all(contrib, ("role", "grp"), split_axis=1, concat_axis=2, tiled=True)
    arrived = arrived.reshape(2, role_count, grp_count, row_share, C).astype(jnp.float32)
    quarter = jnp.sum(arrived, axis=1).astype(jnp.bfloat16)
    collected_rows = lax.all_gather(quarter[:, :, None], "rep", axis=2, tiled=True)
    subgrid = collected_rows.reshape(2, C, C)
    widened = extended(subgrid, ((("role", "grp"), 2),), EDGE)
    residual, regrid = degrid(
        widened, patch_pos[0], counts[0], vis_u[0], vis_v[0], observed[:, 0], kernel
    )
    left_part = regrid[:, :, :EDGE]
    right_part = regrid[:, :, EDGE + C :]
    center = regrid[:, :, EDGE : EDGE + C]
    from_right = shifted(left_part.astype(jnp.bfloat16), ("role", "grp"), -1).astype(
        left_part.dtype
    )
    from_left = shifted(right_part.astype(jnp.bfloat16), ("role", "grp"), 1).astype(
        right_part.dtype
    )
    resid = center.at[:, :, :EDGE].add(from_left).at[:, :, C - EDGE :].add(from_right)
    pieces = resid.reshape(2, grp_count * rep_count, row_share, C)
    spread = lax.all_to_all(
        pieces.astype(jnp.bfloat16), ("grp", "rep"), split_axis=1, concat_axis=1, tiled=True
    ).astype(pieces.dtype)
    owned = jnp.sum(spread.reshape(2, grp_count, rep_count, row_share, C), axis=2).astype(
        jnp.bfloat16
    )
    returned = lax.all_gather(owned, "role", axis=1, tiled=True)
    return (residual[:, None], returned)


LANES = 128
HALF = PATCH // 2
SLOTS = LANES // (2 * HALF)
TURN = 8
EVERYONE = ("role", "grp", "rep")


def lanes_of(shape):
    return lax.broadcasted_iota(jnp.int32, shape, len(shape) - 1)


def sublanes_of(shape):
    return lax.broadcasted_iota(jnp.int32, shape, len(shape) - 2)


def near(value):
    return pltpu.with_memory_space_constraint(value, pltpu.VMEM)


def far(value):
    return pltpu.with_memory_space_constraint(value, pltpu.HBM)


def waves(cells, scale):
    angles = np.arange(C)[:, None] * cells[None, :] % F * (2.0 * np.pi / F)
    return np.stack([np.cos(angles) * scale, np.sin(angles) * scale]).astype(np.float32)


def row_tables():
    cells = np.arange(LANES)
    return waves(cells, 1.0 / math.sqrt(F)), waves(np.full(LANES, LANES), 1.0)


def column_tables():
    cells = np.arange(LANES) % (LANES // 2) * TURN
    return waves(cells, 1.0 / math.sqrt(F)), waves(np.ones(LANES, np.int64), 1.0)


def eighth(index):
    def cosine(turn):
        turn = turn & 7
        size = jnp.where((turn & 1) == 1, math.sqrt(0.5), jnp.where((turn & 3) == 0, 1.0, 0.0))
        return jnp.where((turn > 2) & (turn < 6), -size, size).astype(jnp.float32)

    return cosine(index), cosine(index + 6)


def rotated(cos, sin, turn_cos, turn_sin):
    return cos * turn_cos - sin * turn_sin, sin * turn_cos + cos * turn_sin


def place_kernel(positions, place, copies):
    col_blocks = (C + 2 * EDGE) // PATCH
    slot = (lanes_of((1, LANES)) // HALF) % SLOTS
    value = jnp.zeros((1, LANES), jnp.int32)
    for p in range(SLOTS):
        value = jnp.where(slot == p, positions[0:1, p : p + 1], value)
    row = sum(jnp.where(value >= block * col_blocks, 1, 0) for block in range(1, C // PATCH))
    value = row * (8 - col_blocks) + value
    place[...] = value
    copies[...] = jnp.broadcast_to(value[None], copies.shape)


def row_kernel(
    rep_count, facets, taper, start, turn, keep, send, data, table_a, table_b,
    wave, total, strip, first_rows, second_rows, sems,
):
    chunks, _, width = table_a.shape
    count = keep.shape[0]

    def fetch(chunk):
        columns = pl.ds(pl.multiple_of(chunk * width, width), width)
        return pltpu.make_async_copy(
            facets.at[0, :, :, columns], data.at[chunk], sems.at[chunk]
        )

    fetch(0).start()
    fetch(1).start()
    wave[...] = start[...]
    total[...] = jnp.zeros_like(total)

    def build(step, carry):
        chunk, piece = step // (width // LANES), step % (width // LANES)
        window = taper[:, pl.ds(pl.multiple_of(step * LANES, LANES), LANES)]
        columns = pl.ds(pl.multiple_of(piece * LANES, LANES), LANES)
        for block in range(C // HALF):
            rows = slice(block * HALF, (block + 1) * HALF)
            cos, sin = wave[0, rows, :], wave[1, rows, :]
            re = window * cos
            im = window * sin
            base = (block % 2) * C + (block // 2) * HALF
            low = slice(base, base + HALF)
            high = slice(base + C // 2, base + C // 2 + HALF)
            table_a[chunk, low, columns] = re.astype(jnp.bfloat16)
            table_a[chunk, high, columns] = (-im).astype(jnp.bfloat16)
            table_b[chunk, low, columns] = im.astype(jnp.bfloat16)
            table_b[chunk, high, columns] = re.astype(jnp.bfloat16)
            cos, sin = rotated(cos, sin, turn[0, rows, :], turn[1, rows, :])
            wave[0, rows, :] = cos
            wave[1, rows, :] = sin
        return carry

    lax.fori_loop(0, chunks * (width // LANES), build, 0)

    def multiply(chunk, carry):
        fetch(chunk).wait()

        @pl.when(chunk + 2 < chunks)
        def _():
            fetch(chunk + 2).start()

        total[...] += contract(data[chunk, 0], table_a[chunk]) + contract(
            data[chunk, 1], table_b[chunk]
        )
        return carry

    lax.fori_loop(0, chunks, multiply, 0)
    place = lax.axis_index("grp") * rep_count + lax.axis_index("rep")
    for piece in range(count // LANES):
        offset = pl.multiple_of(place * count + piece * LANES, LANES)
        strip[piece : piece + 1, :] = taper[:, pl.ds(offset, LANES)]
    window = jnp.transpose(strip[...])
    for piece in range(count // LANES):
        rows = slice(piece * LANES, (piece + 1) * LANES)
        scaled = total[rows, :] * window[:, piece : piece + 1]
        first_rows[rows, :] = scaled[:, :C]
        second_rows[rows, :] = scaled[:, C:]
    even = lax.rem(lax.axis_index("rep"), 2) == 0
    part = count // TURN
    for turned in range(TURN):
        rows = pl.ds(turned, part, stride=TURN)
        first, second = first_rows[rows, :], second_rows[rows, :]
        target = slice(turned * part, (turned + 1) * part)
        keep[target, :] = jnp.where(even, first, second).astype(jnp.bfloat16)
        send[target, :] = jnp.where(even, second, first).astype(jnp.bfloat16)


def column_kernel(rep_count, keep, other, start, turn, sub, base, data, groups):
    part = keep.shape[0] // TURN
    mine = lax.axis_index("grp") * rep_count + lax.axis_index("rep")
    near_by = mine + 1 - 2 * lax.rem(mine, 2)
    shape = (HALF, LANES)
    right = lanes_of((1, LANES)) >= LANES // 2
    place = jnp.where(lanes_of(shape) < LANES // 2, mine, near_by)
    phase_cos, phase_sin = eighth((sublanes_of(shape) & 7) * place)
    for block in range(C // HALF):
        rows = slice(block * HALF, (block + 1) * HALF)
        cos, sin = rotated(start[0, rows, :], start[1, rows, :], phase_cos, phase_sin)
        for turned in range(TURN):
            base[turned, rows, :LANES] = cos.astype(jnp.bfloat16)
            base[turned, rows, LANES:] = sin.astype(jnp.bfloat16)
            if turned < TURN - 1:
                cos, sin = rotated(cos, sin, turn[0, rows, :], turn[1, rows, :])
    for turned in range(TURN):
        source = slice(turned * part, (turned + 1) * part)
        for side, ref in enumerate((keep, other)):
            value = ref[source, :]
            swapped = pltpu.roll(value.astype(jnp.float32), LANES // 2, 1)
            data[turned, side * part : (side + 1) * part, :] = value
            data[turned, (2 + side) * part : (3 + side) * part, :] = jnp.where(
                right, -swapped, swapped
            ).astype(jnp.bfloat16)
    for turned in range(TURN):
        groups[turned] = jnp.dot(base[turned], data[turned], preferred_element_type=jnp.float32)

    def quarter(value):
        swapped = pltpu.roll(value, LANES // 2, 1)
        return jnp.where(right, -swapped, swapped)

    def fourths(values):
        low, high = values[0] + values[2], values[0] - values[2]
        odd, turned = values[1] + values[3], quarter(values[1] - values[3])
        return low + odd, high + turned, low - odd, high - turned

    zero = jnp.zeros((EDGE, LANES), jnp.float32)
    sub[:EDGE, :] = zero
    sub[EDGE + TURN * C :, :] = zero
    size = math.sqrt(0.5)
    for block in range(C // HALF):
        rows = slice(block * HALF, (block + 1) * HALF)
        evens = fourths([groups[turned, rows, :] for turned in range(0, TURN, 2)])
        odds = fourths([groups[turned, rows, :] for turned in range(1, TURN, 2)])
        second, fourth = quarter(odds[1]), quarter(odds[3])
        twisted = (
            odds[0],
            (odds[1] + second) * size,
            quarter(odds[2]),
            (fourth - odds[3]) * size,
        )
        for column in range(TURN // 2):
            for sign in range(2):
                value = evens[column] - twisted[column] if sign else evens[column] + twisted[column]
                begin = EDGE + (column + sign * TURN // 2) * C + block * HALF
                sub[begin : begin + HALF, :] = value


def pack_kernel(rep_count, places, sub, out):
    col_blocks = (C + 2 * EDGE) // PATCH
    lane = lanes_of((PATCH, LANES))
    fixed = lane - (lane // HALF) % SLOTS * HALF

    def pack(column, carry):
        begin = pl.multiple_of(column * C, C)
        blocks = [sub[pl.ds(begin + block * PATCH, PATCH), :] for block in range(col_blocks)]
        for rep in range(rep_count):
            mark = jnp.broadcast_to(places[column * rep_count + rep], (PATCH, LANES))
            source, wanted = fixed + (mark >> 3) * HALF, mark & 7
            total = jnp.zeros((PATCH, LANES), jnp.float32)
            for block in range(col_blocks):
                moved = jnp.take_along_axis(blocks[block], source, axis=1)
                total = jnp.where(wanted == block, moved, total)
            out[column * rep_count + rep] = total.astype(jnp.bfloat16)
        return carry

    lax.fori_loop(0, out.shape[0] // rep_count, pack, 0, unroll=True)


def taps_kernel(taps, vis_u, vis_v, taps_u, taps_v):
    length = vis_u.shape[-1]
    taps_u[...] = jnp.zeros_like(taps_u)

    def taps_of(offsets):
        distance = sublanes_of((PATCH, length)) - offsets
        value = jnp.zeros((PATCH, length), jnp.float32)
        for position in range(KW):
            value = jnp.where(distance == position, taps[position], value)
        return value

    for p in range(SLOTS):
        span = slice(p * length, (p + 1) * length)
        rows_u = taps_of(vis_u[0, p : p + 1, :])
        high = rows_u.astype(jnp.bfloat16)
        low = (rows_u - high.astype(jnp.float32)).astype(jnp.bfloat16)
        for half in range(2):
            begin = half * (LANES // 2) + p * HALF
            taps_u[begin : begin + HALF, span] = high[half * HALF : (half + 1) * HALF]
            taps_u[LANES + begin : LANES + begin + HALF, span] = low[
                half * HALF : (half + 1) * HALF
            ]
        taps_v[:, span] = taps_of(vis_v[0, p : p + 1, :])


def degrid_kernel(counts, place, arrived, observed, taps_u, taps_v, residual, out, weighted):
    length = observed.shape[-1]
    left = lanes_of((PATCH, LANES)) < LANES // 2
    sums = []
    for half in range(2):
        total = arrived[half].astype(jnp.float32)
        for source in range(half + 2, arrived.shape[0], 2):
            total = total + arrived[source].astype(jnp.float32)
        sums.append(total)
    swapped = [pltpu.roll(total, LANES // 2, 1) for total in sums]
    patch = jnp.concatenate(
        [jnp.where(left, sums[0], swapped[1]), jnp.where(left, swapped[0], sums[1])], axis=0
    ).astype(jnp.bfloat16)
    patch = jnp.concatenate([patch, patch], axis=1)
    for p in range(SLOTS):
        span = slice(p * length, (p + 1) * length)
        inner = jnp.dot(patch, taps_u[:, span], preferred_element_type=jnp.float32)
        rows_v = taps_v[:, span]
        live = lanes_of((1, length)) < counts[0:1, p : p + 1]
        for c in range(2):
            predicted = jnp.sum(inner[c * PATCH : (c + 1) * PATCH] * rows_v, axis=0, keepdims=True)
            value = jnp.where(live, observed[c, 0, p : p + 1, :] - predicted, 0.0)
            residual[c, 0, p : p + 1, :] = value
            value = value * rows_v
            high = value.astype(jnp.bfloat16)
            weighted[c * PATCH : (c + 1) * PATCH, span] = high
            weighted[2 * PATCH + c * PATCH : 2 * PATCH + (c + 1) * PATCH, span] = (
                value - high.astype(jnp.float32)
            ).astype(jnp.bfloat16)
    product = contract(weighted[...], taps_u[...])
    product = product[: 2 * PATCH] + product[2 * PATCH :]
    gridded = product[:, :LANES] + product[:, LANES:]
    parts = [gridded[:PATCH], gridded[PATCH:]]
    swapped = [pltpu.roll(part, LANES // 2, 1) for part in parts]
    halves = [jnp.where(left, parts[0], swapped[1]), jnp.where(left, swapped[0], parts[1])]
    row = place[...] >> 3
    owners = C // HALF
    for owner in range(owners):
        piece = jnp.where(row == owner // 2, halves[owner % 2], 0.0).astype(jnp.bfloat16)
        for first in range(0, out.shape[0], owners):
            out[first + owner] = piece


def return_kernel(
    rep_count, places, arrived, residual_near, residual, returned_far, canvas, returned, sem, sems
):
    copies = [pltpu.make_async_copy(residual_near, residual, sem)]
    copies[0].start()
    sub_cols = returned.shape[1]
    col_blocks = (C + 2 * EDGE) // PATCH
    for column in range(sub_cols):
        values, marks = [], []
        for rep in range(rep_count):
            device = column * rep_count + rep
            values.append(arrived[device].astype(jnp.float32))
            marks.append(places[device] & 7)
        for block in range(col_blocks):
            total = jnp.where(marks[0] == block, values[0], 0.0)
            for value, mark in zip(values[1:], marks[1:]):
                total = total + jnp.where(mark == block, value, 0.0)
            canvas[column * col_blocks + block] = total
    shape = (2 * HALF, LANES)
    row, lane = sublanes_of(shape), lanes_of(shape)
    picked = (row // HALF == lane // (LANES // 2)) & (row % HALF == lane % HALF)
    pick = jnp.where(picked, 1.0, 0.0).astype(jnp.bfloat16)
    pick = jnp.concatenate([pick, pick], axis=1)
    for column in range(sub_cols):
        blocks = [canvas[column * col_blocks + 1 + block] for block in range(C // PATCH)]
        if column > 0:
            blocks[0] = blocks[0] + canvas[column * col_blocks - 1]
        if column < sub_cols - 1:
            blocks[-1] = blocks[-1] + canvas[(column + 1) * col_blocks]
        total = jnp.concatenate(blocks, axis=0)
        high = total.astype(jnp.bfloat16)
        low = (total - high.astype(jnp.float32)).astype(jnp.bfloat16)
        value = contract(pick, jnp.concatenate([high, low], axis=1)).astype(jnp.bfloat16)
        for c in range(2):
            returned[c, column] = value[c * HALF : (c + 1) * HALF]
        if column % 2 == 1:
            columns = slice(column - 1, column + 1)
            copies.append(
                pltpu.make_async_copy(
                    returned.at[:, columns], returned_far.at[:, columns], sems.at[column // 2]
                )
            )
            copies[-1].start()
    for copy in copies:
        copy.wait()


def call(kernel, out_shape, operands, scratch, flops, scalars=0, first=None, outs=None, limit=24):
    spaces = [pltpu.SMEM] * scalars + [pltpu.VMEM] * (len(operands) - scalars)
    if first is not None:
        spaces[0] = first
    single = not isinstance(out_shape, tuple)
    outs = outs or (pltpu.VMEM,) * (1 if single else len(out_shape))
    specs = tuple(pl.BlockSpec(memory_space=space) for space in outs)
    return pl.pallas_call(
        kernel,
        out_shape=out_shape,
        in_specs=[pl.BlockSpec(memory_space=space) for space in spaces],
        out_specs=specs[0] if single else specs,
        scratch_shapes=scratch,
        compiler_params=pltpu.CompilerParams(vmem_limit_bytes=limit << 20),
        cost_estimate=pl.CostEstimate(flops=flops, bytes_accessed=1 << 20, transcendentals=0),
    )(*operands)


def exchanged(value):
    return lax.all_to_all(value, EVERYONE, split_axis=0, concat_axis=0, tiled=True)


def fused(facets, taper, kernel, observed, patch_pos, counts, vis_u, vis_v):
    rep_count = lax.axis_size("rep")
    sub_cols = lax.axis_size("role") * lax.axis_size("grp")
    devices = sub_cols * rep_count
    count = facets.shape[2]
    length = observed.shape[-1]
    chunks = 4
    col_blocks = (C + 2 * EDGE) // PATCH
    f32, bf16 = jnp.float32, jnp.bfloat16

    place, copies = call(
        place_kernel,
        (pltpu.VMEM((1, LANES), jnp.int32), pltpu.VMEM((devices, 1, LANES), jnp.int32)),
        (patch_pos,),
        [],
        1 << 33,
    )
    places = exchanged(copies)
    places = near(places)
    strip = pltpu.VMEM((count, LANES), bf16)
    keep, send = call(
        lambda *refs: row_kernel(rep_count, *refs),
        (strip, strip),
        (far(facets), near(taper)) + tuple(near(jnp.asarray(table)) for table in row_tables()),
        [
            pltpu.VMEM((chunks, 2, count, F // chunks), bf16),
            pltpu.VMEM((chunks, 2 * C, F // chunks), bf16),
            pltpu.VMEM((chunks, 2 * C, F // chunks), bf16),
            pltpu.VMEM((2, C, LANES), f32),
            pltpu.VMEM((count, 2 * C), f32),
            pltpu.VMEM((8, LANES), f32),
            pltpu.VMEM((count, LANES), f32),
            pltpu.VMEM((count, LANES), f32),
            pltpu.SemaphoreType.DMA((chunks,)),
        ],
        8 * C * F * count,
        first=pltpu.HBM,
    )
    pairs = [(i, i + 1 - 2 * (i % 2)) for i in range(rep_count)]
    other = lax.ppermute(send, "rep", pairs)
    other = near(other)
    taps_u, taps_v = call(
        taps_kernel,
        (
            pltpu.VMEM((2 * LANES, SLOTS * length), bf16),
            pltpu.VMEM((PATCH, SLOTS * length), f32),
        ),
        (kernel, near(vis_u), near(vis_v)),
        [],
        1 << 26,
        scalars=1,
    )
    sub = call(
        lambda *refs: column_kernel(rep_count, *refs),
        pltpu.VMEM((sub_cols * C + 2 * EDGE, LANES), f32),
        (near(keep), other) + tuple(near(table) for table in column_tables()),
        [
            pltpu.VMEM((TURN, C, 2 * LANES), bf16),
            pltpu.VMEM((TURN, 2 * LANES, LANES), bf16),
            pltpu.VMEM((TURN, C, LANES), f32),
        ],
        1 << 20,
    )
    chunk = pltpu.VMEM((devices, PATCH, LANES), bf16)
    outgoing = call(
        lambda *refs: pack_kernel(rep_count, *refs), chunk, (places, near(sub)), [], 1 << 28
    )
    arrived = near(exchanged(outgoing))
    residual, gridded = call(
        degrid_kernel,
        (pltpu.VMEM(observed.shape, f32), chunk),
        (near(counts), place, arrived, near(observed), near(taps_u), near(taps_v)),
        [pltpu.VMEM((4 * PATCH, SLOTS * length), bf16)],
        1 << 28,
    )
    spread = near(exchanged(gridded))
    return call(
        lambda *refs: return_kernel(rep_count, *refs),
        (
            pltpu.HBM(observed.shape, f32),
            pltpu.HBM((2, sub_cols, HALF, C), bf16),
        ),
        (places, spread, near(residual)),
        [
            pltpu.VMEM((sub_cols * col_blocks, PATCH, LANES), f32),
            pltpu.VMEM((2, sub_cols, HALF, C), bf16),
            pltpu.SemaphoreType.DMA,
            pltpu.SemaphoreType.DMA((sub_cols // 2,)),
        ],
        1 << 26,
        outs=(pltpu.HBM, pltpu.HBM),
    )


def part(facets, taper, kernel, observed, patch_pos, counts, vis_u, vis_v):
    grp_count = lax.axis_size("grp")
    rep_count = lax.axis_size("rep")
    owners = grp_count * rep_count
    sub_cols = lax.axis_size("role") * grp_count
    whole = (
        owners * HALF == C
        and owners == TURN
        and sub_cols == TURN
        and facets.shape[2] * TURN == F
        and rep_count % 2 == 0
        and patch_pos.shape[1] == SLOTS
        and facets.shape[2] == TURN * LANES // 2
        and observed.shape[-1] % LANES == 0
    )
    path = fused if whole else local
    return path(facets, taper, kernel, observed, patch_pos, counts, vis_u, vis_v)


def solution(mesh):
    return jax.shard_map(
        part,
        mesh=mesh,
        in_specs=(
            P("role", None, ("grp", "rep"), None),
            P("role", None),
            P(),
            P(None, ("role", "grp"), "rep", None),
            P(("role", "grp"), "rep"),
            P(("role", "grp"), "rep"),
            P(("role", "grp"), "rep", None),
            P(("role", "grp"), "rep", None),
        ),
        out_specs=(P(None, ("role", "grp"), "rep", None), P(None, None, ("grp", "rep"), None)),
        check_vma=False,
    )
```
